256 devices in a mesh: member: 16 (over z, y_hi), band: 16 (over y_lo, x, core).
Axes of the slice: x: 4, y: 4 (y_hi: 2, y_lo: 2; y = y_hi * 2 + y_lo), z: 8, core: 2. Of those that a mesh axis runs over, the one named last changes fastest.
Arguments:
- spectral: float32 [256, 768, 768], P('member', 'band'), parts along dimension 0, may hold values from -6 to 6
- coupling: float32 [16384, 1024], P(('member', 'band')), parts along dimension 0, may hold values from 0.02 to 162, as said below
- quadratic: float32 [16384, 1024], P(('member', 'band')), parts along dimension 0, may hold values from -1.5 to 1.5
Outputs:
- tendency_spectral: float32 [256, 768, 768], P('member', 'band'), parts along dimension 0
The draws below stay inside these ranges and needn't reach their ends.
There are 16 independent parts, one for each index of `member`. The reference program is written for one: setup_inputs(seed, part) draws one part's arguments, and reference() takes and returns one part's arrays. A program takes and returns all parts, laid end to end along the dimension named above; each array names one. Nothing has to cross between parts.
Inputs may be any that keep to these rules, and one draw needn't show every extreme that they name: `coupling`: positive.
All inputs are finite; a program needn't handle non-finite values.
Results may differ from the reference program's by a relative error of at most 0.00008.
Values sent between devices are 32-bit elements; how exact they have to be, the bound alone decides.
A program may use at most 128 MiB of HBM per device.

```python
import math
import jax
import jax.numpy as jnp
from jax import lax

N = 1024
LEVELS = 16
KS = 768


def draw_coupling(key, part):
    keys = jax.random.split(jax.random.fold_in(key, 11), 3)
    rows = jnp.arange(N, dtype=jnp.float32) / N
    row_noise = jax.random.uniform(keys[0], (N,), jnp.float32)
    col_noise = jax.random.uniform(keys[1], (N,), jnp.float32)
    trend = jnp.exp(jnp.log(3.0) * rows)
    cell = jax.random.uniform(keys[2], (N, N), jnp.float32, 0.5, 1.5)
    row_scale = trend * jnp.exp(jnp.log(10.0) * row_noise)
    col_scale = jnp.exp(jnp.log(10.0) * col_noise)
    return (row_scale[:, None] * col_scale[None, :] * cell / 10.0).astype(jnp.float32)


def block_levels(stream_key, extent, shards, smallest, largest):
    def one(dim, shards_of):
        steps = jax.random.uniform(jax.random.fold_in(jax.random.fold_in(stream_key, 6), dim), (shards_of,), jnp.float32, smallest / len(shards), largest / len(shards))
        return jnp.repeat(jnp.exp(steps), extent[dim] // shards_of).reshape((-1,) + (1,) * (len(extent) - dim - 1))

    gain = one(*shards[0])
    for cut in shards[1:]:
        gain = gain * one(*cut)
    return gain


def noise(stream_key, shape, deviation, most, cuts=(), kind=jnp.bfloat16):
    result = deviation * jax.random.normal(stream_key, shape, jnp.float32)
    if cuts:
        result = result * block_levels(stream_key, shape, cuts, -0.22, 0.18)
    return jnp.clip(result, -most, most).astype(kind)


def setup_inputs(seed: int = 0, part: int = 0) -> dict:
    seeds = jax.random.split(jax.random.key(seed), 4)
    part_splits = jax.random.split(jax.random.fold_in(seeds[3], part), 4)
    spectral = noise(part_splits[0], (LEVELS, KS, KS), 1.0, 6.0, ((1, 16),), jnp.float32)
    coupling = draw_coupling(jax.random.fold_in(jax.random.fold_in(seeds[3], part), 71), part)
    quadratic = noise(part_splits[2], (N, N), 0.25, 1.5, ((0, 16),), jnp.float32)
    return {"spectral": spectral, "coupling": coupling, "quadratic": quadratic}


def tables(cells, coeffs):
    half_count = coeffs // 2
    position = jnp.arange(cells, dtype=jnp.int32)
    column = jnp.arange(coeffs, dtype=jnp.int32)
    wavenumber = jnp.where(column < half_count, column, column - half_count)
    turns = position[:, None] * wavenumber[None, :] % cells
    angles = turns.astype(jnp.float32) * (2.0 * math.pi / cells)
    basis_table = jnp.where(column[None, :] < half_count, jnp.cos(angles), jnp.sin(angles))
    synthesis = basis_table / math.sqrt(half_count)
    factor = jnp.where(wavenumber == 0, 1.0, 2.0) * (math.sqrt(half_count) / cells)
    analysis = (basis_table * factor[None, :]).T
    return (synthesis, analysis)

def reference(spectral, coupling, quadratic):
    synthesis, analysis = tables(N, KS)
    high = lax.Precision.HIGHEST
    section = jnp.einsum('lab,yb->lay', spectral, synthesis, precision=high)
    grid = jnp.einsum('xa,lay->lyx', synthesis, section, precision=high)
    product = coupling[None] * grid
    energy = lax.optimization_barrier(jnp.mean(product * product, axis=(1, 2)))
    scaled = product / jnp.sqrt(energy + 1e-06)[:, None, None]
    tendency = scaled + quadratic[None] * scaled * scaled
    back = jnp.einsum('ax,lyx->lya', analysis, tendency, precision=high)
    return jnp.einsum('by,lya->lab', analysis, back, precision=high)
```

```python
import functools
import math

import jax
import jax.numpy as jnp
import numpy as np
from jax import lax
from jax.experimental import pallas as pl
from jax.experimental.pallas import tpu as pltpu
from jax.sharding import PartitionSpec as P

MESH = pl.DeviceIdType.MESH
F32 = jnp.float32
BF16 = jnp.bfloat16
GROUP = 4
LANES = 128


def small_tables(cells, coeffs):
    half = coeffs // 2
    k = np.arange(half)
    q = np.arange(LANES)
    fine = 2.0 * math.pi / cells * (k[:, None] * q[None, :] % cells)
    steps = np.arange(cells // LANES)
    coarse = 2.0 * math.pi / cells * (steps[:, None] * LANES * k[None, :] % cells)
    by_k = np.stack([np.cos(fine), np.sin(fine)])
    by_q = np.stack([np.cos(fine.T), np.sin(fine.T)])
    row = np.stack([np.cos(coarse), np.sin(coarse)])
    column = np.repeat(row[:, :, :8, None], LANES, axis=3)
    return tuple(a.astype(np.float32) for a in (by_k, by_q, row, column))


def split(value):
    high = value.astype(BF16)
    return high, (value - high.astype(F32)).astype(BF16)


def dot3(a_high, a_low, b_high, b_low):
    dot = functools.partial(jnp.dot, preferred_element_type=F32)
    return dot(a_high, b_high) + dot(a_low, b_high) + dot(a_high, b_low)


def kernel(
    n,
    spectral,
    coupling,
    quadratic,
    by_k,
    by_q,
    row,
    column,
    out,
    x_in,
    send1,
    recv1,
    product,
    send2,
    recv2,
    result,
    part_out,
    part_in,
    wide_high,
    wide_low,
    tall_high,
    tall_low,
    gain,
    bend,
    left_high,
    left_low,
    right_high,
    right_low,
    in_sem,
    out_sem,
    send1_sem,
    recv1_sem,
    send2_sem,
    recv2_sem,
    part_send_sem,
    part_recv_sem,
):
    chunks, band, coeffs = x_in.shape[0], send1.shape[2], x_in.shape[2]
    half = coeffs // 2
    rows, cells = coupling.shape
    points = float(cells * cells)
    wide = GROUP * rows
    me = lax.axis_index("band")

    for c in range(chunks):
        pltpu.make_async_copy(spectral.at[c], x_in.at[c], in_sem.at[c]).start()

    barrier = pltpu.get_barrier_semaphore()

    @pl.loop(1, n)
    def _(k):
        pl.semaphore_signal(
            barrier, inc=1, device_id={"band": lax.rem(me + k, n)}, device_id_type=MESH
        )

    for step in range(cells // LANES):
        lanes = pl.ds(step * LANES, LANES)
        cos_q = by_k[0].reshape(half // 8, 8, LANES)
        sin_q = by_k[1].reshape(half // 8, 8, LANES)
        cos_s, sin_s = column[0, step][None], column[1, step][None]
        cosine = (cos_q * cos_s - sin_q * sin_s).reshape(half, LANES)
        sine = (sin_q * cos_s + cos_q * sin_s).reshape(half, LANES)
        wide_high[pl.ds(0, half), lanes], wide_low[pl.ds(0, half), lanes] = split(cosine)
        wide_high[pl.ds(half, half), lanes], wide_low[pl.ds(half, half), lanes] = split(sine)

    pl.semaphore_wait(barrier, n - 1)

    low_half = lax.broadcasted_iota(jnp.int32, (band, LANES), 1) < rows

    def send(source, target, c, send_sem, recv_sem):
        @pl.loop(1, n)
        def _(k):
            other = lax.rem(me + k, n)
            pltpu.make_async_remote_copy(
                src_ref=source.at[c, other],
                dst_ref=target.at[c, me],
                send_sem=send_sem.at[c],
                recv_sem=recv_sem.at[c],
                device_id={"band": other},
                device_id_type=MESH,
            ).start()
        target[c, me] = source[c, me]

    def arrivals(source, target, c, send_sem, recv_sem):
        others = pl.ds(0, n - 1)
        return pltpu.make_async_remote_copy(
            src_ref=source.at[c, others],
            dst_ref=target.at[c, others],
            send_sem=send_sem.at[c],
            recv_sem=recv_sem.at[c],
            device_id={"band": lax.rem(me + 1, n)},
            device_id_type=MESH,
        )

    first = (send1, recv1)
    second = (send2, recv2)

    @pl.loop(0, chunks)
    def _(c):
        pltpu.make_async_copy(spectral.at[c], x_in.at[c], in_sem.at[c]).wait()
        x_high, x_low = split(x_in[c])
        for j in range(cells // wide):
            lanes = pl.ds(j * wide, wide)
            section = dot3(x_high, x_low, wide_high[:, lanes], wide_low[:, lanes])
            for level in range(0, GROUP, 2):
                for t in range(wide // LANES):
                    part = slice(t * LANES, (t + 1) * LANES)
                    even = section[level * band : (level + 1) * band, part]
                    odd = section[(level + 1) * band : (level + 2) * band, part]
                    target = 2 * (j * (wide // LANES) + t)
                    place = pl.ds(level * rows, LANES)
                    send1[c, target, :, place] = jnp.where(
                        low_half, even, pltpu.roll(odd, rows, 1)
                    )
                    send1[c, target + 1, :, place] = jnp.where(
                        low_half, pltpu.roll(even, rows, 1), odd
                    )

        @pl.when(c < 2)
        def _():
            send(*first, c, send1_sem, recv1_sem)

    for step in range(cells // LANES):
        points_here = pl.ds(step * LANES, LANES)
        cos_s, sin_s = row[0, pl.ds(step, 1)], row[1, pl.ds(step, 1)]
        cosine = by_q[0] * cos_s - by_q[1] * sin_s
        sine = by_q[1] * cos_s + by_q[0] * sin_s
        (tall_high[points_here, pl.ds(0, half)], tall_low[points_here, pl.ds(0, half)]) = split(
            cosine
        )
        (
            tall_high[points_here, pl.ds(half, half)],
            tall_low[points_here, pl.ds(half, half)],
        ) = split(sine)

    for step in range(cells // LANES):
        here = pl.ds(step * LANES, LANES)
        field = coupling[:, here] * (1.0 / half)
        gain[here, :] = jnp.concatenate([field, field], axis=0).T
        field = quadratic[:, here]
        bend[here, :] = jnp.concatenate([field, field], axis=0).T

    def synthesize(c):
        arrivals(*first, c, send1_sem, recv1_sem).wait_recv()
        right_high[pl.ds(0, coeffs)], right_low[pl.ds(0, coeffs)] = split(
            recv1[c].reshape(coeffs, wide)
        )
        grid = dot3(
            tall_high[...],
            tall_low[...],
            right_high[pl.ds(0, coeffs)],
            right_low[pl.ds(0, coeffs)],
        )
        for t in range(wide // LANES):
            lanes = slice(t * LANES, (t + 1) * LANES)
            value = gain[...] * grid[:, lanes]
            product[c, :, lanes] = value
            part_out[c, pl.ds(t, 1), :] = jnp.sum(value * value, axis=0, keepdims=True)

        @pl.loop(1, n)
        def _(k):
            other = lax.rem(me + k, n)
            pltpu.make_async_remote_copy(
                src_ref=part_out.at[c],
                dst_ref=part_in.at[c, me],
                send_sem=part_send_sem.at[c],
                recv_sem=part_recv_sem.at[c],
                device_id={"band": other},
                device_id_type=MESH,
            ).start()
        part_in[c, me] = part_out[c]

    def analyze(c):
        others = pl.ds(0, n - 1)
        done = pltpu.make_async_remote_copy(
            src_ref=part_in.at[c, others],
            dst_ref=part_in.at[c, others],
            send_sem=part_send_sem.at[c],
            recv_sem=part_recv_sem.at[c],
            device_id={"band": lax.rem(me + 1, n)},
            device_id_type=MESH,
        )
        done.wait_recv()
        sums = part_in[c, 0]
        for source in range(1, n):
            sums = sums + part_in[c, source]
        left = lax.broadcasted_iota(jnp.int32, sums.shape, 1) < rows
        total = jnp.where(
            left,
            jnp.sum(jnp.where(left, sums, 0.0), axis=1, keepdims=True),
            jnp.sum(jnp.where(left, 0.0, sums), axis=1, keepdims=True),
        )
        scale = 1.0 / jnp.sqrt(total * (1.0 / points) + 1e-06)
        for t in range(wide // LANES):
            lanes = slice(t * LANES, (t + 1) * LANES)
            scaled = product[c, :, lanes] * scale[t : t + 1]
            tendency = scaled + bend[...] * scaled * scaled
            right_high[:, lanes], right_low[:, lanes] = split(tendency)
        back = dot3(wide_high[...], wide_low[...], right_high[...], right_low[...])
        send2[c] = back.reshape(n, band, wide)
        send(*second, c, send2_sem, recv2_sem)

    x_index = lax.broadcasted_iota(jnp.int32, (band, coeffs), 0) + me * band
    y_index = lax.broadcasted_iota(jnp.int32, (band, coeffs), 1)

    def weight(index):
        return jnp.where((index == 0) | (index == half), 1.0, 2.0)

    def finish(c):
        arrivals(*second, c, send2_sem, recv2_sem).wait_recv()
        for level in range(0, GROUP, 2):
            place = pl.ds(level * rows, LANES)
            for t in range(cells // LANES):
                lanes = pl.ds(t * LANES, LANES)
                even = recv2[c, 2 * t, :, place]
                odd = recv2[c, 2 * t + 1, :, place]
                for which, value in (
                    (level, jnp.where(low_half, even, pltpu.roll(odd, rows, 1))),
                    (level + 1, jnp.where(low_half, pltpu.roll(even, rows, 1), odd)),
                ):
                    here = pl.ds(which * band, band)
                    left_high[here, lanes], left_low[here, lanes] = split(value)
        done = dot3(left_high[...], left_low[...], tall_high[...], tall_low[...])
        factor = weight(x_index) * weight(y_index) * (half / points)
        for level in range(GROUP):
            here = slice(level * band, (level + 1) * band)
            result[c, here, :] = done[here] * factor
        pltpu.make_async_copy(result.at[c], out.at[c], out_sem.at[c]).start()

    @pl.loop(0, chunks + 3)
    def _(t):
        @pl.when(t < chunks)
        def _():
            synthesize(t)

        @pl.when(t + 2 < chunks)
        def _():
            send(*first, t + 2, send1_sem, recv1_sem)

        @pl.when((t >= 1) & (t < chunks + 1))
        def _():
            analyze(t - 1)

        @pl.when(t >= 3)
        def _():
            finish(t - 3)

    @pl.loop(0, chunks)
    def _(c):
        arrivals(*first, c, send1_sem, recv1_sem).wait_send()
        arrivals(*second, c, send2_sem, recv2_sem).wait_send()
        others = pl.ds(0, n - 1)
        pltpu.make_async_remote_copy(
            src_ref=part_in.at[c, others],
            dst_ref=part_in.at[c, others],
            send_sem=part_send_sem.at[c],
            recv_sem=part_recv_sem.at[c],
            device_id={"band": lax.rem(me + 1, n)},
            device_id_type=MESH,
        ).wait_send()
        pltpu.make_async_copy(result.at[c], out.at[c], out_sem.at[c]).wait()


def solution(mesh):
    n = mesh.shape["band"]

    def on_device(spectral, coupling, quadratic):
        levels, band, coeffs = spectral.shape
        rows, cells = coupling.shape
        chunks = levels // GROUP
        wide = GROUP * rows
        tables = small_tables(cells, coeffs)
        dma = pltpu.SemaphoreType.DMA
        vmem = pl.BlockSpec(memory_space=pltpu.VMEM)
        hbm = pl.BlockSpec(memory_space=pl.ANY)
        result = pl.pallas_call(
            functools.partial(kernel, n),
            out_shape=jax.ShapeDtypeStruct((chunks, GROUP * band, coeffs), F32),
            in_specs=[hbm] + [vmem] * 6,
            out_specs=hbm,
            scratch_shapes=[
                pltpu.VMEM((chunks, GROUP * band, coeffs), F32),
                pltpu.VMEM((chunks, n, band, wide), F32),
                pltpu.VMEM((chunks, n, band, wide), F32),
                pltpu.VMEM((chunks, cells, wide), F32),
                pltpu.VMEM((chunks, n, band, wide), F32),
                pltpu.VMEM((chunks, n, band, wide), F32),
                pltpu.VMEM((chunks, GROUP * band, coeffs), F32),
                pltpu.VMEM((chunks, wide // LANES, LANES), F32),
                pltpu.VMEM((chunks, n, wide // LANES, LANES), F32),
                pltpu.VMEM((coeffs, cells), BF16),
                pltpu.VMEM((coeffs, cells), BF16),
                pltpu.VMEM((cells, coeffs), BF16),
                pltpu.VMEM((cells, coeffs), BF16),
                pltpu.VMEM((cells, LANES), F32),
                pltpu.VMEM((cells, LANES), F32),
                pltpu.VMEM((GROUP * band, cells), BF16),
                pltpu.VMEM((GROUP * band, cells), BF16),
                pltpu.VMEM((cells, wide), BF16),
                pltpu.VMEM((cells, wide), BF16),
            ]
            + [dma((chunks,))] * 8,
            compiler_params=pltpu.CompilerParams(
                collective_id=0, has_side_effects=True, vmem_limit_bytes=56 * 1024 * 1024
            ),
        )(spectral.reshape(chunks, GROUP * band, coeffs), coupling, quadratic, *tables)
        return result.reshape(levels, band, coeffs)

    spec = P("member", "band", None)
    field = P(("member", "band"), None)
    return jax.shard_map(
        on_device,
        mesh=mesh,
        in_specs=(spec, field, field),
        out_specs=spec,
        check_vma=False,
    )
```

```python
import functools
import math

import jax
import jax.numpy as jnp
from jax import lax
from jax.experimental import pallas as pl
from jax.experimental.pallas import tpu as pltpu
from jax.sharding import PartitionSpec as P

MESH = pl.DeviceIdType.MESH
F32 = jnp.float32
BF16 = jnp.bfloat16
GROUP = 4
LANES = 128


SINE = (-1.6666666666666666e-01, 8.3333333333333333e-03, -1.9841269841269841e-04, 2.7557319223985891e-06)
COSINE = (-0.5, 4.1666666666666667e-02, -1.3888888888888889e-03, 2.4801587301587302e-05, -2.7557319223985891e-07)


def turn(index, cells):
    quarter = cells // 4
    index = lax.rem(index, cells)
    which = index // quarter
    angle = (index - which * quarter - quarter // 2).astype(F32) * (2.0 * math.pi / cells)
    square = angle * angle

    def series(terms):
        total = terms[-1]
        for term in terms[-2::-1]:
            total = total * square + term
        return total * square + 1.0

    cosine = series(COSINE) * math.sqrt(0.5)
    sine = series(SINE) * angle * math.sqrt(0.5)
    plus, minus = cosine + sine, cosine - sine
    cos_sign = jnp.where((which == 1) | (which == 2), -1.0, 1.0)
    sin_sign = jnp.where(which >= 2, -1.0, 1.0)
    odd = (which == 1) | (which == 3)
    return jnp.where(odd, plus, minus) * cos_sign, jnp.where(odd, minus, plus) * sin_sign


def split(value):
    high = value.astype(BF16)
    return high, (value - high.astype(F32)).astype(BF16)


def dot3(a_high, a_low, b_high, b_low):
    dot = functools.partial(jnp.dot, preferred_element_type=F32)
    return dot(a_high, b_high) + dot(a_low, b_high) + dot(a_high, b_low)


def kernel(
    n,
    spectral,
    coupling_hbm,
    quadratic_hbm,
    out,
    x_in,
    coupling,
    quadratic,
    send1,
    recv1,
    product,
    send2,
    recv2,
    part_out,
    part_in,
    wide_high,
    wide_low,
    tall_high,
    tall_low,
    gain,
    bend,
    left_high,
    left_low,
    right_high,
    right_low,
    in_sem,
    field_sem,
    send1_sem,
    recv1_sem,
    send2_sem,
    recv2_sem,
    part_send_sem,
    part_recv_sem,
):
    chunks, band, coeffs = x_in.shape[0], send1.shape[2], x_in.shape[2]
    half = coeffs // 2
    rows, cells = coupling.shape
    points = float(cells * cells)
    wide = GROUP * rows
    me = lax.axis_index("band")

    for c in range(chunks):
        pltpu.make_async_copy(spectral.at[c], x_in.at[c], in_sem.at[c]).start()
    pltpu.make_async_copy(coupling_hbm, coupling, field_sem.at[0]).start()
    pltpu.make_async_copy(quadratic_hbm, quadratic, field_sem.at[1]).start()

    barrier = pltpu.get_barrier_semaphore()

    @pl.loop(1, n)
    def _(k):
        pl.semaphore_signal(
            barrier, inc=1, device_id={"band": lax.rem(me + k, n)}, device_id_type=MESH
        )

    def count(shape, axis):
        return lax.broadcasted_iota(jnp.int32, shape, axis)

    fine = (half, LANES)
    cos_q, sin_q = turn(count(fine, 0) * count(fine, 1), cells)
    cos_q = cos_q.reshape(half // 8, 8, LANES)
    sin_q = sin_q.reshape(half // 8, 8, LANES)
    for step in range(cells // LANES):
        lanes = pl.ds(step * LANES, LANES)
        cos_s, sin_s = turn(count((8, LANES), 0) * (step * LANES), cells)
        cos_s, sin_s = cos_s[None], sin_s[None]
        cosine = (cos_q * cos_s - sin_q * sin_s).reshape(half, LANES)
        sine = (sin_q * cos_s + cos_q * sin_s).reshape(half, LANES)
        wide_high[pl.ds(0, half), lanes], wide_low[pl.ds(0, half), lanes] = split(cosine)
        wide_high[pl.ds(half, half), lanes], wide_low[pl.ds(half, half), lanes] = split(sine)

    low_half = lax.broadcasted_iota(jnp.int32, (band, LANES), 1) < rows

    def send_one(source, target, c, send_sem, recv_sem, other):
        pltpu.make_async_remote_copy(
            src_ref=source.at[c, other],
            dst_ref=target.at[c, me],
            send_sem=send_sem.at[c],
            recv_sem=recv_sem.at[c],
            device_id={"band": other},
            device_id_type=MESH,
        ).start()

    def send(source, target, c, send_sem, recv_sem):
        @pl.loop(1, n)
        def _(k):
            send_one(source, target, c, send_sem, recv_sem, lax.rem(me + k, n))
        target[c, me] = source[c, me]

    def arrivals(source, target, c, send_sem, recv_sem):
        others = pl.ds(0, n - 1)
        return pltpu.make_async_remote_copy(
            src_ref=source.at[c, others],
            dst_ref=target.at[c, others],
            send_sem=send_sem.at[c],
            recv_sem=recv_sem.at[c],
            device_id={"band": lax.rem(me + 1, n)},
            device_id_type=MESH,
        )

    first = (send1, recv1)
    second = (send2, recv2)

    @pl.loop(0, chunks)
    def _(c):
        pltpu.make_async_copy(spectral.at[c], x_in.at[c], in_sem.at[c]).wait()
        x_high, x_low = split(x_in[c])
        per = wide // rows

        @pl.loop(0, cells // wide)
        def _(turned):
            j = lax.rem(turned + me // per + 1, cells // wide)
            lanes = pl.ds(pl.multiple_of(j * wide, wide), wide)
            section = dot3(x_high, x_low, wide_high[:, lanes], wide_low[:, lanes])
            for level in range(0, GROUP, 2):
                for t in range(wide // LANES):
                    part = slice(t * LANES, (t + 1) * LANES)
                    even = section[level * band : (level + 1) * band, part]
                    odd = section[(level + 1) * band : (level + 2) * band, part]
                    target = j * per + 2 * t
                    place = pl.ds(level * rows, LANES)
                    send1[c, target, :, place] = jnp.where(
                        low_half, even, pltpu.roll(odd, rows, 1)
                    )
                    send1[c, target + 1, :, place] = jnp.where(
                        low_half, pltpu.roll(even, rows, 1), odd
                    )

            @pl.when((c == 0) & (turned == 0))
            def _():
                pl.semaphore_wait(barrier, n - 1)

            @pl.when(c < 2)
            def _():
                @pl.loop(0, per)
                def _(i):
                    other = j * per + i

                    @pl.when(other != me)
                    def _():
                        send_one(*first, c, send1_sem, recv1_sem, other)

        @pl.when(c < 2)
        def _():
            recv1[c, me] = send1[c, me]

    fine = (LANES, half)
    cos_q, sin_q = turn(count(fine, 0) * count(fine, 1), cells)
    for step in range(cells // LANES):
        points_here = pl.ds(step * LANES, LANES)
        cos_s, sin_s = turn(count((8, half), 1) * (step * LANES), cells)
        cos_s, sin_s = cos_s[:1], sin_s[:1]
        cosine = cos_q * cos_s - sin_q * sin_s
        sine = sin_q * cos_s + cos_q * sin_s
        (tall_high[points_here, pl.ds(0, half)], tall_low[points_here, pl.ds(0, half)]) = split(
            cosine
        )
        (
            tall_high[points_here, pl.ds(half, half)],
            tall_low[points_here, pl.ds(half, half)],
        ) = split(sine)

    pltpu.make_async_copy(coupling_hbm, coupling, field_sem.at[0]).wait()
    pltpu.make_async_copy(quadratic_hbm, quadratic, field_sem.at[1]).wait()

    for step in range(cells // LANES):
        here = pl.ds(step * LANES, LANES)
        field = coupling[:, here] * (1.0 / half)
        gain[here, :] = jnp.concatenate([field, field], axis=0).T
        field = quadratic[:, here]
        bend[here, :] = jnp.concatenate([field, field], axis=0).T

    def synthesize(c):
        arrivals(*first, c, send1_sem, recv1_sem).wait_recv()
        right_high[pl.ds(0, coeffs)], right_low[pl.ds(0, coeffs)] = split(
            recv1[c].reshape(coeffs, wide)
        )
        grid = dot3(
            tall_high[...],
            tall_low[...],
            right_high[pl.ds(0, coeffs)],
            right_low[pl.ds(0, coeffs)],
        )
        for t in range(wide // LANES):
            lanes = slice(t * LANES, (t + 1) * LANES)
            value = gain[...] * grid[:, lanes]
            product[c, :, lanes] = value
            part_out[c, pl.ds(t, 1), :] = jnp.sum(value * value, axis=0, keepdims=True)

        @pl.loop(1, n)
        def _(k):
            other = lax.rem(me + k, n)
            pltpu.make_async_remote_copy(
                src_ref=part_out.at[c],
                dst_ref=part_in.at[c, me],
                send_sem=part_send_sem.at[c],
                recv_sem=part_recv_sem.at[c],
                device_id={"band": other},
                device_id_type=MESH,
            ).start()
        part_in[c, me] = part_out[c]

    def analyze(c):
        others = pl.ds(0, n - 1)
        done = pltpu.make_async_remote_copy(
            src_ref=part_in.at[c, others],
            dst_ref=part_in.at[c, others],
            send_sem=part_send_sem.at[c],
            recv_sem=part_recv_sem.at[c],
            device_id={"band": lax.rem(me + 1, n)},
            device_id_type=MESH,
        )
        done.wait_recv()
        sums = part_in[c, 0]
        for source in range(1, n):
            sums = sums + part_in[c, source]
        left = lax.broadcasted_iota(jnp.int32, sums.shape, 1) < rows
        total = jnp.where(
            left,
            jnp.sum(jnp.where(left, sums, 0.0), axis=1, keepdims=True),
            jnp.sum(jnp.where(left, 0.0, sums), axis=1, keepdims=True),
        )
        scale = 1.0 / jnp.sqrt(total * (1.0 / points) + 1e-06)
        for t in range(wide // LANES):
            lanes = slice(t * LANES, (t + 1) * LANES)
            scaled = product[c, :, lanes] * scale[t : t + 1]
            tendency = scaled + bend[...] * scaled * scaled
            right_high[:, lanes], right_low[:, lanes] = split(tendency)
        back = dot3(wide_high[...], wide_low[...], right_high[...], right_low[...])
        send2[c] = back.reshape(n, band, wide)
        send(*second, c, send2_sem, recv2_sem)

    x_index = lax.broadcasted_iota(jnp.int32, (band, coeffs), 0) + me * band
    y_index = lax.broadcasted_iota(jnp.int32, (band, coeffs), 1)

    def weight(index):
        return jnp.where((index == 0) | (index == half), 1.0, 2.0)

    def finish(c):
        arrivals(*second, c, send2_sem, recv2_sem).wait_recv()
        for level in range(0, GROUP, 2):
            place = pl.ds(level * rows, LANES)
            for t in range(cells // LANES):
                lanes = pl.ds(t * LANES, LANES)
                even = recv2[c, 2 * t, :, place]
                odd = recv2[c, 2 * t + 1, :, place]
                for which, value in (
                    (level, jnp.where(low_half, even, pltpu.roll(odd, rows, 1))),
                    (level + 1, jnp.where(low_half, pltpu.roll(even, rows, 1), odd)),
                ):
                    here = pl.ds(which * band, band)
                    left_high[here, lanes], left_low[here, lanes] = split(value)
        done = dot3(left_high[...], left_low[...], tall_high[...], tall_low[...])
        factor = weight(x_index) * weight(y_index) * (half / points)
        for level in range(GROUP):
            here = slice(level * band, (level + 1) * band)
            out[c, here, :] = done[here] * factor

    @pl.loop(0, chunks + 3)
    def _(t):
        @pl.when(t < chunks)
        def _():
            synthesize(t)

        @pl.when(t + 2 < chunks)
        def _():
            send(*first, t + 2, send1_sem, recv1_sem)

        @pl.when((t >= 1) & (t < chunks + 1))
        def _():
            analyze(t - 1)

        @pl.when(t >= 3)
        def _():
            finish(t - 3)

    @pl.loop(0, chunks)
    def _(c):
        arrivals(*first, c, send1_sem, recv1_sem).wait_send()
        arrivals(*second, c, send2_sem, recv2_sem).wait_send()
        others = pl.ds(0, n - 1)
        pltpu.make_async_remote_copy(
            src_ref=part_in.at[c, others],
            dst_ref=part_in.at[c, others],
            send_sem=part_send_sem.at[c],
            recv_sem=part_recv_sem.at[c],
            device_id={"band": lax.rem(me + 1, n)},
            device_id_type=MESH,
        ).wait_send()


def solution(mesh):
    n = mesh.shape["band"]

    def on_device(spectral, coupling, quadratic):
        levels, band, coeffs = spectral.shape
        rows, cells = coupling.shape
        chunks = levels // GROUP
        wide = GROUP * rows
        dma = pltpu.SemaphoreType.DMA
        vmem = pl.BlockSpec(memory_space=pltpu.VMEM)
        hbm = pl.BlockSpec(memory_space=pltpu.HBM)
        result = pl.pallas_call(
            functools.partial(kernel, n),
            out_shape=pltpu.VMEM((chunks, GROUP * band, coeffs), F32),
            in_specs=[hbm] * 3,
            out_specs=vmem,
            scratch_shapes=[
                pltpu.VMEM((chunks, GROUP * band, coeffs), F32),
                pltpu.VMEM((rows, cells), F32),
                pltpu.VMEM((rows, cells), F32),
                pltpu.VMEM((chunks, n, band, wide), F32),
                pltpu.VMEM((chunks, n, band, wide), F32),
                pltpu.VMEM((chunks, cells, wide), F32),
                pltpu.VMEM((chunks, n, band, wide), F32),
                pltpu.VMEM((chunks, n, band, wide), F32),
                pltpu.VMEM((chunks, wide // LANES, LANES), F32),
                pltpu.VMEM((chunks, n, wide // LANES, LANES), F32),
                pltpu.VMEM((coeffs, cells), BF16),
                pltpu.VMEM((coeffs, cells), BF16),
                pltpu.VMEM((cells, coeffs), BF16),
                pltpu.VMEM((cells, coeffs), BF16),
                pltpu.VMEM((cells, LANES), F32),
                pltpu.VMEM((cells, LANES), F32),
                pltpu.VMEM((GROUP * band, cells), BF16),
                pltpu.VMEM((GROUP * band, cells), BF16),
                pltpu.VMEM((cells, wide), BF16),
                pltpu.VMEM((cells, wide), BF16),
            ]
            + [dma((chunks,)), dma((2,))] + [dma((chunks,))] * 6,
            compiler_params=pltpu.CompilerParams(
                collective_id=0, has_side_effects=True, vmem_limit_bytes=44 * 1024 * 1024
            ),
        )(
            *(
                pltpu.with_memory_space_constraint(value, pltpu.HBM)
                for value in (spectral.reshape(chunks, GROUP * band, coeffs), coupling, quadratic)
            )
        )
        return result.reshape(levels, band, coeffs)

    spec = P("member", "band", None)
    field = P(("member", "band"), None)
    return jax.shard_map(
        on_device,
        mesh=mesh,
        in_specs=(spec, field, field),
        out_specs=spec,
        check_vma=False,
    )
```

```python
import functools
import math

import jax
import jax.numpy as jnp
from jax import lax
from jax.experimental import pallas as pl
from jax.experimental.pallas import tpu as pltpu
from jax.sharding import PartitionSpec as P

MESH = pl.DeviceIdType.MESH
F32 = jnp.float32
BF16 = jnp.bfloat16
GROUP = 2
AHEAD = 3
ANALYZE = 3
FINISH = 6
LANES = 128
ORDER = ((1, 2), (0, 1), (1, 3), (0, 2), (1, 0), (0, 3), (1, 1), (0, 0))


SINE = (-1.6666666666666666e-01, 8.3333333333333333e-03, -1.9841269841269841e-04, 2.7557319223985891e-06)
COSINE = (-0.5, 4.1666666666666667e-02, -1.3888888888888889e-03, 2.4801587301587302e-05, -2.7557319223985891e-07)


def turn(index, cells):
    quarter = cells // 4
    index = lax.rem(index, cells)
    which = index // quarter
    angle = (index - which * quarter - quarter // 2).astype(F32) * (2.0 * math.pi / cells)
    square = angle * angle

    def series(terms):
        total = terms[-1]
        for term in terms[-2::-1]:
            total = total * square + term
        return total * square + 1.0

    cosine = series(COSINE) * math.sqrt(0.5)
    sine = series(SINE) * angle * math.sqrt(0.5)
    plus, minus = cosine + sine, cosine - sine
    cos_sign = jnp.where((which == 1) | (which == 2), -1.0, 1.0)
    sin_sign = jnp.where(which >= 2, -1.0, 1.0)
    odd = (which == 1) | (which == 3)
    return jnp.where(odd, plus, minus) * cos_sign, jnp.where(odd, minus, plus) * sin_sign


def split(value):
    high = value.astype(BF16)
    return high, (value - high.astype(F32)).astype(BF16)


def dot3(a_high, a_low, b_high, b_low):
    dot = functools.partial(jnp.dot, preferred_element_type=F32)
    return dot(a_high, b_high) + dot(a_low, b_high) + dot(a_high, b_low)


def kernel(
    n,
    spectral,
    coupling_hbm,
    quadratic_hbm,
    out,
    x_in,
    coupling,
    quadratic,
    send1,
    recv1,
    product,
    send2,
    recv2,
    part_out,
    part_in,
    wide_high,
    wide_low,
    tall_high,
    tall_low,
    gain,
    bend,
    left_high,
    left_low,
    right_high,
    right_low,
    down_high,
    down_low,
    in_sem,
    field_sem,
    send1_sem,
    recv1_sem,
    send2_sem,
    recv2_sem,
    part_send_sem,
    part_recv_sem,
):
    chunks, band, coeffs = x_in.shape[0], send1.shape[2], x_in.shape[2]
    half = coeffs // 2
    rows, cells = coupling.shape
    points = float(cells * cells)
    fold = cells // 2
    wide = GROUP * rows
    me = lax.axis_index("band")
    chip, core = me // 2, lax.rem(me, 2)
    ring = n // 4

    def at(dy, dx, dc):
        y, x = lax.rem(chip // ring + dy, 2), lax.rem(chip + dx, ring)
        return 2 * (ring * y + x) + lax.rem(core + dc, 2)

    others = [at(dy, dx, dc) for dy, dx in ORDER for dc in range(2) if (dy, dx, dc) != (0, 0, 0)]

    for c in range(chunks):
        pltpu.make_async_copy(spectral.at[c], x_in.at[c], in_sem.at[c]).start()
    pltpu.make_async_copy(coupling_hbm, coupling, field_sem.at[0]).start()
    pltpu.make_async_copy(quadratic_hbm, quadratic, field_sem.at[1]).start()

    barrier = pltpu.get_barrier_semaphore()

    @pl.loop(1, n)
    def _(k):
        pl.semaphore_signal(
            barrier, inc=1, device_id={"band": lax.rem(me + k, n)}, device_id_type=MESH
        )

    def count(shape, axis):
        return lax.broadcasted_iota(jnp.int32, shape, axis)

    fine = (half, LANES)
    cos_q, sin_q = turn(count(fine, 0) * count(fine, 1), cells)
    cos_q = cos_q.reshape(half // 8, 8, LANES)
    sin_q = sin_q.reshape(half // 8, 8, LANES)
    for step in range(fold // LANES):
        lanes = pl.ds(step * LANES, LANES)
        cos_s, sin_s = turn(count((8, LANES), 0) * (step * LANES), cells)
        cos_s, sin_s = cos_s[None], sin_s[None]
        cosine = (cos_q * cos_s - sin_q * sin_s).reshape(half, LANES)
        sine = (sin_q * cos_s + cos_q * sin_s).reshape(half, LANES)
        wide_high[pl.ds(0, half), lanes], wide_low[pl.ds(0, half), lanes] = split(cosine)
        wide_high[pl.ds(half, half), lanes], wide_low[pl.ds(half, half), lanes] = split(sine)

    low_half = lax.broadcasted_iota(jnp.int32, (band, LANES), 1) < rows

    def send_one(source, target, c, send_sem, recv_sem, other):
        pltpu.make_async_remote_copy(
            src_ref=source.at[c, other],
            dst_ref=target.at[c, me],
            send_sem=send_sem.at[c],
            recv_sem=recv_sem.at[c],
            device_id={"band": other},
            device_id_type=MESH,
        ).start()

    def send(source, target, c, send_sem, recv_sem):
        for other in others:
            send_one(source, target, c, send_sem, recv_sem, other)
        target[c, me] = source[c, me]

    def arrivals(source, target, c, send_sem, recv_sem):
        rest = pl.ds(0, n - 1)
        return pltpu.make_async_remote_copy(
            src_ref=source.at[c, rest],
            dst_ref=target.at[c, rest],
            send_sem=send_sem.at[c],
            recv_sem=recv_sem.at[c],
            device_id={"band": lax.rem(me + 1, n)},
            device_id_type=MESH,
        )

    first = (send1, recv1)
    second = (send2, recv2)

    @pl.loop(0, chunks)
    def _(c):
        pltpu.make_async_copy(spectral.at[c], x_in.at[c], in_sem.at[c]).wait()
        value = x_in[c]
        even_k = lax.rem(count(value.shape, 1), 2) == 0
        parts = jnp.concatenate([jnp.where(even_k, value, 0.0), jnp.where(even_k, 0.0, value)])
        x_high, x_low = split(parts)
        tile = 2 * LANES
        for j in range(fold // tile):
            lanes = pl.ds(j * tile, tile)
            both = dot3(x_high, x_low, wide_high[:, lanes], wide_low[:, lanes])
            even_sum, odd_sum = both[: GROUP * band], both[GROUP * band :]
            for side, section in enumerate((even_sum + odd_sum, even_sum - odd_sum)):
                for level in range(0, GROUP, 2):
                    for t in range(tile // LANES):
                        part = slice(t * LANES, (t + 1) * LANES)
                        even = section[level * band : (level + 1) * band, part]
                        odd = section[(level + 1) * band : (level + 2) * band, part]
                        target = (side * fold + j * tile + t * LANES) // rows
                        place = pl.ds(level * rows, LANES)
                        send1[c, target, :, place] = jnp.where(
                            low_half, even, pltpu.roll(odd, rows, 1)
                        )
                        send1[c, target + 1, :, place] = jnp.where(
                            low_half, pltpu.roll(even, rows, 1), odd
                        )

        @pl.when(c == 0)
        def _():
            pl.semaphore_wait(barrier, n - 1)

        @pl.when(c < AHEAD)
        def _():
            send(*first, c, send1_sem, recv1_sem)

    fine = (LANES, half)
    cos_q, sin_q = turn(count(fine, 0) * count(fine, 1), cells)
    for step in range(fold // LANES):
        points_here = pl.ds(step * LANES, LANES)
        cos_s, sin_s = turn(count((8, half), 1) * (step * LANES), cells)
        cos_s, sin_s = cos_s[:1], sin_s[:1]
        cosine = cos_q * cos_s - sin_q * sin_s
        sine = sin_q * cos_s + cos_q * sin_s
        (tall_high[points_here, pl.ds(0, half)], tall_low[points_here, pl.ds(0, half)]) = split(
            cosine
        )
        (
            tall_high[points_here, pl.ds(half, half)],
            tall_low[points_here, pl.ds(half, half)],
        ) = split(sine)

    pltpu.make_async_copy(coupling_hbm, coupling, field_sem.at[0]).wait()
    pltpu.make_async_copy(quadratic_hbm, quadratic, field_sem.at[1]).wait()

    for step in range(cells // LANES):
        here = pl.ds(step * LANES, LANES)
        field = coupling[:, here] * (1.0 / half)
        gain[here, :] = jnp.concatenate([field, field], axis=0).T
        field = quadratic[:, here]
        bend[here, :] = jnp.concatenate([field, field], axis=0).T

    def synthesize(c):
        arrivals(*first, c, send1_sem, recv1_sem).wait_recv()
        value = recv1[c].reshape(coeffs, wide)
        even_k = lax.rem(count(value.shape, 0), 2) == 0
        for side, part in enumerate((jnp.where(even_k, value, 0.0), jnp.where(even_k, 0.0, value))):
            lanes = pl.ds(side * wide, wide)
            right_high[:, lanes], right_low[:, lanes] = split(part)
        both = dot3(tall_high[...], tall_low[...], right_high[...], right_low[...])
        even_sum, odd_sum = both[:, :wide], both[:, wide:]
        sums = 0.0
        for side, grid in enumerate((even_sum + odd_sum, even_sum - odd_sum)):
            here = pl.ds(side * fold, fold)
            value = jnp.concatenate([gain[here]] * (wide // LANES), axis=1) * grid
            product[c, here] = value
            sums = sums + jnp.sum(value * value, axis=0, keepdims=True)
        for t in range(wide // LANES):
            part_out[c, pl.ds(t, 1), :] = sums[:, t * LANES : (t + 1) * LANES]

        for other in others:
            pltpu.make_async_remote_copy(
                src_ref=part_out.at[c],
                dst_ref=part_in.at[c, me],
                send_sem=part_send_sem.at[c],
                recv_sem=part_recv_sem.at[c],
                device_id={"band": other},
                device_id_type=MESH,
            ).start()
        part_in[c, me] = part_out[c]

    def analyze(c):
        rest = pl.ds(0, n - 1)
        done = pltpu.make_async_remote_copy(
            src_ref=part_in.at[c, rest],
            dst_ref=part_in.at[c, rest],
            send_sem=part_send_sem.at[c],
            recv_sem=part_recv_sem.at[c],
            device_id={"band": lax.rem(me + 1, n)},
            device_id_type=MESH,
        )
        done.wait_recv()
        sums = part_in[c, 0]
        for source in range(1, n):
            sums = sums + part_in[c, source]
        left = lax.broadcasted_iota(jnp.int32, sums.shape, 1) < rows
        total = jnp.where(
            left,
            jnp.sum(jnp.where(left, sums, 0.0), axis=1, keepdims=True),
            jnp.sum(jnp.where(left, 0.0, sums), axis=1, keepdims=True),
        )
        scale = 1.0 / jnp.sqrt(total * (1.0 / points) + 1e-06)
        scale = jnp.concatenate([scale[t : t + 1] for t in range(wide // LANES)], axis=1)
        halves = []
        for side in range(2):
            here = pl.ds(side * fold, fold)
            scaled = product[c, here] * scale
            weight = jnp.concatenate([bend[here]] * (wide // LANES), axis=1)
            halves.append(scaled + weight * scaled * scaled)
        for side, part in enumerate((halves[0] + halves[1], halves[0] - halves[1])):
            lanes = pl.ds(side * wide, wide)
            down_high[:, lanes], down_low[:, lanes] = split(part)
        both = dot3(wide_high[...], wide_low[...], down_high[...], down_low[...])
        even_k = lax.rem(count((coeffs, wide), 0), 2) == 0
        back = jnp.where(even_k, both[:, :wide], both[:, wide:])
        send2[c] = back.reshape(n, band, wide)
        send(*second, c, send2_sem, recv2_sem)

    x_index = lax.broadcasted_iota(jnp.int32, (band, coeffs), 0) + me * band
    y_index = lax.broadcasted_iota(jnp.int32, (band, coeffs), 1)

    def weight(index):
        return jnp.where((index == 0) | (index == half), 1.0, 2.0)

    def finish(c):
        arrivals(*second, c, send2_sem, recv2_sem).wait_recv()
        for level in range(0, GROUP, 2):
            place = pl.ds(level * rows, LANES)
            for t in range(fold // LANES):
                lanes = pl.ds(t * LANES, LANES)
                turned = []
                for near in (2 * t, 2 * t + fold // rows):
                    even = recv2[c, near, :, place]
                    odd = recv2[c, near + 1, :, place]
                    turned.append(
                        (
                            jnp.where(low_half, even, pltpu.roll(odd, rows, 1)),
                            jnp.where(low_half, pltpu.roll(even, rows, 1), odd),
                        )
                    )
                for which in range(2):
                    near, far = turned[0][which], turned[1][which]
                    here = (level + which) * band
                    for side, value in enumerate((near + far, near - far)):
                        there = pl.ds(side * GROUP * band + here, band)
                        left_high[there, lanes], left_low[there, lanes] = split(value)
        both = dot3(left_high[...], left_low[...], tall_high[...], tall_low[...])
        even_k = lax.rem(count((GROUP * band, coeffs), 1), 2) == 0
        done = jnp.where(even_k, both[: GROUP * band], both[GROUP * band :])
        factor = weight(x_index) * weight(y_index) * (half / points)
        for level in range(GROUP):
            here = slice(level * band, (level + 1) * band)
            out[c, here, :] = done[here] * factor

    @pl.loop(0, chunks + FINISH)
    def _(t):
        @pl.when(t < chunks)
        def _():
            synthesize(t)

        @pl.when(t + AHEAD < chunks)
        def _():
            send(*first, t + AHEAD, send1_sem, recv1_sem)

        @pl.when((t >= ANALYZE) & (t < chunks + ANALYZE))
        def _():
            analyze(t - ANALYZE)

        @pl.when(t >= FINISH)
        def _():
            finish(t - FINISH)

    @pl.loop(0, chunks)
    def _(c):
        arrivals(*first, c, send1_sem, recv1_sem).wait_send()
        arrivals(*second, c, send2_sem, recv2_sem).wait_send()
        rest = pl.ds(0, n - 1)
        pltpu.make_async_remote_copy(
            src_ref=part_in.at[c, rest],
            dst_ref=part_in.at[c, rest],
            send_sem=part_send_sem.at[c],
            recv_sem=part_recv_sem.at[c],
            device_id={"band": lax.rem(me + 1, n)},
            device_id_type=MESH,
        ).wait_send()


def solution(mesh):
    n = mesh.shape["band"]

    def on_device(spectral, coupling, quadratic):
        levels, band, coeffs = spectral.shape
        rows, cells = coupling.shape
        chunks = levels // GROUP
        wide = GROUP * rows
        dma = pltpu.SemaphoreType.DMA
        vmem = pl.BlockSpec(memory_space=pltpu.VMEM)
        hbm = pl.BlockSpec(memory_space=pltpu.HBM)
        result = pl.pallas_call(
            functools.partial(kernel, n),
            out_shape=pltpu.VMEM((chunks, GROUP * band, coeffs), F32),
            in_specs=[hbm] * 3,
            out_specs=vmem,
            scratch_shapes=[
                pltpu.VMEM((chunks, GROUP * band, coeffs), F32),
                pltpu.VMEM((rows, cells), F32),
                pltpu.VMEM((rows, cells), F32),
                pltpu.VMEM((chunks, n, band, wide), F32),
                pltpu.VMEM((chunks, n, band, wide), F32),
                pltpu.VMEM((chunks, cells, wide), F32),
                pltpu.VMEM((chunks, n, band, wide), F32),
                pltpu.VMEM((chunks, n, band, wide), F32),
                pltpu.VMEM((chunks, wide // LANES, LANES), F32),
                pltpu.VMEM((chunks, n, wide // LANES, LANES), F32),
                pltpu.VMEM((coeffs, cells // 2), BF16),
                pltpu.VMEM((coeffs, cells // 2), BF16),
                pltpu.VMEM((cells // 2, coeffs), BF16),
                pltpu.VMEM((cells // 2, coeffs), BF16),
                pltpu.VMEM((cells, LANES), F32),
                pltpu.VMEM((cells, LANES), F32),
                pltpu.VMEM((2 * GROUP * band, cells // 2), BF16),
                pltpu.VMEM((2 * GROUP * band, cells // 2), BF16),
                pltpu.VMEM((coeffs, 2 * wide), BF16),
                pltpu.VMEM((coeffs, 2 * wide), BF16),
                pltpu.VMEM((cells // 2, 2 * wide), BF16),
                pltpu.VMEM((cells // 2, 2 * wide), BF16),
            ]
            + [dma((chunks,)), dma((2,))] + [dma((chunks,))] * 6,
            compiler_params=pltpu.CompilerParams(
                collective_id=0, has_side_effects=True, vmem_limit_bytes=44 * 1024 * 1024
            ),
        )(
            *(
                pltpu.with_memory_space_constraint(value, pltpu.HBM)
                for value in (spectral.reshape(chunks, GROUP * band, coeffs), coupling, quadratic)
            )
        )
        return result.reshape(levels, band, coeffs)

    spec = P("member", "band", None)
    field = P(("member", "band"), None)
    return jax.shard_map(
        on_device,
        mesh=mesh,
        in_specs=(spec, field, field),
        out_specs=spec,
        check_vma=False,
    )
```

```python
import functools
import math

import jax
import jax.numpy as jnp
from jax import lax
from jax.experimental import pallas as pl
from jax.experimental.pallas import tpu as pltpu
from jax.sharding import PartitionSpec as P

MESH = pl.DeviceIdType.MESH
F32 = jnp.float32
BF16 = jnp.bfloat16
GROUP = 2
AHEAD = 3
ANALYZE = 3
FINISH = 6
LANES = 128
ORDER = ((1, 2), (0, 3), (1, 1), (0, 2), (1, 0), (0, 1), (1, 3), (0, 0))


SINE = (-1.6666666666666666e-01, 8.3333333333333333e-03, -1.9841269841269841e-04, 2.7557319223985891e-06)
COSINE = (-0.5, 4.1666666666666667e-02, -1.3888888888888889e-03, 2.4801587301587302e-05, -2.7557319223985891e-07)


def turn(index, cells):
    quarter = cells // 4
    index = lax.rem(index, cells)
    which = index // quarter
    angle = (index - which * quarter - quarter // 2).astype(F32) * (2.0 * math.pi / cells)
    square = angle * angle

    def series(terms):
        total = terms[-1]
        for term in terms[-2::-1]:
            total = total * square + term
        return total * square + 1.0

    cosine = series(COSINE) * math.sqrt(0.5)
    sine = series(SINE) * angle * math.sqrt(0.5)
    plus, minus = cosine + sine, cosine - sine
    cos_sign = jnp.where((which == 1) | (which == 2), -1.0, 1.0)
    sin_sign = jnp.where(which >= 2, -1.0, 1.0)
    odd = (which == 1) | (which == 3)
    return jnp.where(odd, plus, minus) * cos_sign, jnp.where(odd, minus, plus) * sin_sign


def split(value):
    high = value.astype(BF16)
    return high, (value - high.astype(F32)).astype(BF16)


def dot3(a_high, a_low, b_high, b_low):
    dot = functools.partial(jnp.dot, preferred_element_type=F32)
    return dot(a_high, b_high) + dot(a_low, b_high) + dot(a_high, b_low)


def kernel(
    n,
    spectral,
    coupling_hbm,
    quadratic_hbm,
    out,
    x_in,
    coupling,
    quadratic,
    send1,
    recv1,
    product,
    send2,
    recv2,
    part_out,
    part_in,
    wide_high,
    wide_low,
    tall_high,
    tall_low,
    gain,
    bend,
    left_high,
    left_low,
    right_high,
    right_low,
    down_high,
    down_low,
    in_sem,
    field_sem,
    send1_sem,
    recv1_sem,
    send2_sem,
    recv2_sem,
    part_send_sem,
    part_recv_sem,
):
    chunks, band, coeffs = x_in.shape[0], send1.shape[2], x_in.shape[2]
    half = coeffs // 2
    rows, cells = coupling.shape
    points = float(cells * cells)
    fold = cells // 2
    wide = GROUP * rows
    me = lax.axis_index("band")
    chip, core = me // 2, lax.rem(me, 2)
    ring = n // 4

    def at(dy, dx, dc):
        y, x = lax.rem(chip // ring + dy, 2), lax.rem(chip + dx, ring)
        return 2 * (ring * y + x) + lax.rem(core + dc, 2)

    others = [at(dy, dx, dc) for dy, dx in ORDER for dc in range(2) if (dy, dx, dc) != (0, 0, 0)]

    for c in range(chunks):
        pltpu.make_async_copy(spectral.at[c], x_in.at[c], in_sem.at[c]).start()
    pltpu.make_async_copy(coupling_hbm, coupling, field_sem.at[0]).start()
    pltpu.make_async_copy(quadratic_hbm, quadratic, field_sem.at[1]).start()

    barrier = pltpu.get_barrier_semaphore()

    @pl.loop(1, n)
    def _(k):
        pl.semaphore_signal(
            barrier, inc=1, device_id={"band": lax.rem(me + k, n)}, device_id_type=MESH
        )

    def count(shape, axis):
        return lax.broadcasted_iota(jnp.int32, shape, axis)

    fine = (half, LANES)
    cos_q, sin_q = turn(count(fine, 0) * count(fine, 1), cells)
    cos_q = cos_q.reshape(half // 8, 8, LANES)
    sin_q = sin_q.reshape(half // 8, 8, LANES)
    for step in range(fold // LANES):
        lanes = pl.ds(step * LANES, LANES)
        cos_s, sin_s = turn(count((8, LANES), 0) * (step * LANES), cells)
        cos_s, sin_s = cos_s[None], sin_s[None]
        cosine = (cos_q * cos_s - sin_q * sin_s).reshape(half, LANES)
        sine = (sin_q * cos_s + cos_q * sin_s).reshape(half, LANES)
        wide_high[pl.ds(0, half), lanes], wide_low[pl.ds(0, half), lanes] = split(cosine)
        wide_high[pl.ds(half, half), lanes], wide_low[pl.ds(half, half), lanes] = split(sine)

    low_half = lax.broadcasted_iota(jnp.int32, (band, LANES), 1) < rows

    def send_one(source, target, c, send_sem, recv_sem, other):
        pltpu.make_async_remote_copy(
            src_ref=source.at[c, other],
            dst_ref=target.at[c, me],
            send_sem=send_sem.at[c],
            recv_sem=recv_sem.at[c],
            device_id={"band": other},
            device_id_type=MESH,
        ).start()

    def send(source, target, c, send_sem, recv_sem):
        for other in others:
            send_one(source, target, c, send_sem, recv_sem, other)
        target[c, me] = source[c, me]

    def arrivals(source, target, c, send_sem, recv_sem):
        rest = pl.ds(0, n - 1)
        return pltpu.make_async_remote_copy(
            src_ref=source.at[c, rest],
            dst_ref=target.at[c, rest],
            send_sem=send_sem.at[c],
            recv_sem=recv_sem.at[c],
            device_id={"band": lax.rem(me + 1, n)},
            device_id_type=MESH,
        )

    def sums_of(c):
        rest = pl.ds(0, n - 1)
        return pltpu.make_async_remote_copy(
            src_ref=part_in.at[c, rest],
            dst_ref=part_in.at[c, rest],
            send_sem=part_send_sem.at[c],
            recv_sem=part_recv_sem.at[c],
            device_id={"band": lax.rem(me + 1, n)},
            device_id_type=MESH,
        )

    first = (send1, recv1)
    second = (send2, recv2)

    @pl.loop(0, chunks)
    def _(c):
        pltpu.make_async_copy(spectral.at[c], x_in.at[c], in_sem.at[c]).wait()
        value = x_in[c]
        even_k = lax.rem(count(value.shape, 1), 2) == 0
        parts = jnp.concatenate([jnp.where(even_k, value, 0.0), jnp.where(even_k, 0.0, value)])
        x_high, x_low = split(parts)
        tile = 2 * LANES
        for j in range(fold // tile):
            lanes = pl.ds(j * tile, tile)
            both = dot3(x_high, x_low, wide_high[:, lanes], wide_low[:, lanes])
            even_sum, odd_sum = both[: GROUP * band], both[GROUP * band :]
            for side, section in enumerate((even_sum + odd_sum, even_sum - odd_sum)):
                for level in range(0, GROUP, 2):
                    for t in range(tile // LANES):
                        part = slice(t * LANES, (t + 1) * LANES)
                        even = section[level * band : (level + 1) * band, part]
                        odd = section[(level + 1) * band : (level + 2) * band, part]
                        target = (side * fold + j * tile + t * LANES) // rows
                        place = pl.ds(level * rows, LANES)
                        send1[c, target, :, place] = jnp.where(
                            low_half, even, pltpu.roll(odd, rows, 1)
                        )
                        send1[c, target + 1, :, place] = jnp.where(
                            low_half, pltpu.roll(even, rows, 1), odd
                        )

        @pl.when(c == 0)
        def _():
            pl.semaphore_wait(barrier, n - 1)

        @pl.when(c < AHEAD)
        def _():
            send(*first, c, send1_sem, recv1_sem)

    fine = (LANES, half)
    cos_q, sin_q = turn(count(fine, 0) * count(fine, 1), cells)
    for step in range(fold // LANES):
        points_here = pl.ds(step * LANES, LANES)
        cos_s, sin_s = turn(count((8, half), 1) * (step * LANES), cells)
        cos_s, sin_s = cos_s[:1], sin_s[:1]
        cosine = cos_q * cos_s - sin_q * sin_s
        sine = sin_q * cos_s + cos_q * sin_s
        (tall_high[points_here, pl.ds(0, half)], tall_low[points_here, pl.ds(0, half)]) = split(
            cosine
        )
        (
            tall_high[points_here, pl.ds(half, half)],
            tall_low[points_here, pl.ds(half, half)],
        ) = split(sine)

    pltpu.make_async_copy(coupling_hbm, coupling, field_sem.at[0]).wait()
    pltpu.make_async_copy(quadratic_hbm, quadratic, field_sem.at[1]).wait()

    for step in range(cells // LANES):
        here = pl.ds(step * LANES, LANES)
        field = coupling[:, here] * (1.0 / half)
        gain[here, :] = jnp.concatenate([field, field], axis=0).T
        field = quadratic[:, here]
        bend[here, :] = jnp.concatenate([field, field], axis=0).T

    def synthesize(c):
        arrivals(*first, c, send1_sem, recv1_sem).wait_recv()
        value = recv1[c].reshape(coeffs, wide)
        even_k = lax.rem(count(value.shape, 0), 2) == 0
        for side, part in enumerate((jnp.where(even_k, value, 0.0), jnp.where(even_k, 0.0, value))):
            lanes = pl.ds(side * wide, wide)
            right_high[:, lanes], right_low[:, lanes] = split(part)
        both = dot3(tall_high[...], tall_low[...], right_high[...], right_low[...])
        even_sum, odd_sum = both[:, :wide], both[:, wide:]
        sums = 0.0
        for side, grid in enumerate((even_sum + odd_sum, even_sum - odd_sum)):
            here = pl.ds(side * fold, fold)
            value = jnp.concatenate([gain[here]] * (wide // LANES), axis=1) * grid
            product[c, here] = value
            sums = sums + jnp.sum(value * value, axis=0, keepdims=True)
        for t in range(wide // LANES):
            part_out[c, pl.ds(t, 1), :] = sums[:, t * LANES : (t + 1) * LANES]

        for other in others:
            pltpu.make_async_remote_copy(
                src_ref=part_out.at[c],
                dst_ref=part_in.at[c, me],
                send_sem=part_send_sem.at[c],
                recv_sem=part_recv_sem.at[c],
                device_id={"band": other},
                device_id_type=MESH,
            ).start()
        part_in[c, me] = part_out[c]

    def analyze(c):
        sums_of(c).wait_recv()
        sums = part_in[c, 0]
        for source in range(1, n):
            sums = sums + part_in[c, source]
        left = lax.broadcasted_iota(jnp.int32, sums.shape, 1) < rows
        total = jnp.where(
            left,
            jnp.sum(jnp.where(left, sums, 0.0), axis=1, keepdims=True),
            jnp.sum(jnp.where(left, 0.0, sums), axis=1, keepdims=True),
        )
        scale = 1.0 / jnp.sqrt(total * (1.0 / points) + 1e-06)
        scale = jnp.concatenate([scale[t : t + 1] for t in range(wide // LANES)], axis=1)
        halves = []
        for side in range(2):
            here = pl.ds(side * fold, fold)
            scaled = product[c, here] * scale
            weight = jnp.concatenate([bend[here]] * (wide // LANES), axis=1)
            halves.append(scaled + weight * scaled * scaled)
        for side, part in enumerate((halves[0] + halves[1], halves[0] - halves[1])):
            lanes = pl.ds(side * wide, wide)
            down_high[:, lanes], down_low[:, lanes] = split(part)
        both = dot3(wide_high[...], wide_low[...], down_high[...], down_low[...])
        even_k = lax.rem(count((coeffs, wide), 0), 2) == 0
        back = jnp.where(even_k, both[:, :wide], both[:, wide:])
        send2[c] = back.reshape(n, band, wide)
        send(*second, c, send2_sem, recv2_sem)

    x_index = lax.broadcasted_iota(jnp.int32, (band, coeffs), 0) + me * band
    y_index = lax.broadcasted_iota(jnp.int32, (band, coeffs), 1)

    def weight(index):
        return jnp.where((index == 0) | (index == half), 1.0, 2.0)

    def finish(c):
        arrivals(*first, c, send1_sem, recv1_sem).wait_send()
        arrivals(*second, c, send2_sem, recv2_sem).wait_send()
        sums_of(c).wait_send()
        arrivals(*second, c, send2_sem, recv2_sem).wait_recv()
        for level in range(0, GROUP, 2):
            place = pl.ds(level * rows, LANES)
            for t in range(fold // LANES):
                lanes = pl.ds(t * LANES, LANES)
                turned = []
                for near in (2 * t, 2 * t + fold // rows):
                    even = recv2[c, near, :, place]
                    odd = recv2[c, near + 1, :, place]
                    turned.append(
                        (
                            jnp.where(low_half, even, pltpu.roll(odd, rows, 1)),
                            jnp.where(low_half, pltpu.roll(even, rows, 1), odd),
                        )
                    )
                for which in range(2):
                    near, far = turned[0][which], turned[1][which]
                    here = (level + which) * band
                    for side, value in enumerate((near + far, near - far)):
                        there = pl.ds(side * GROUP * band + here, band)
                        left_high[there, lanes], left_low[there, lanes] = split(value)
        both = dot3(left_high[...], left_low[...], tall_high[...], tall_low[...])
        even_k = lax.rem(count((GROUP * band, coeffs), 1), 2) == 0
        done = jnp.where(even_k, both[: GROUP * band], both[GROUP * band :])
        factor = weight(x_index) * weight(y_index) * (half / points)
        for level in range(GROUP):
            here = slice(level * band, (level + 1) * band)
            out[c, here, :] = done[here] * factor

    @pl.loop(0, chunks + FINISH)
    def _(t):
        @pl.when(t < chunks)
        def _():
            synthesize(t)

        @pl.when(t + AHEAD < chunks)
        def _():
            send(*first, t + AHEAD, send1_sem, recv1_sem)

        @pl.when((t >= ANALYZE) & (t < chunks + ANALYZE))
        def _():
            analyze(t - ANALYZE)

        @pl.when(t >= FINISH)
        def _():
            finish(t - FINISH)


def solution(mesh):
    n = mesh.shape["band"]

    def on_device(spectral, coupling, quadratic):
        levels, band, coeffs = spectral.shape
        rows, cells = coupling.shape
        chunks = levels // GROUP
        wide = GROUP * rows
        dma = pltpu.SemaphoreType.DMA
        vmem = pl.BlockSpec(memory_space=pltpu.VMEM)
        hbm = pl.BlockSpec(memory_space=pltpu.HBM)
        result = pl.pallas_call(
            functools.partial(kernel, n),
            out_shape=pltpu.VMEM((chunks, GROUP * band, coeffs), F32),
            in_specs=[hbm] * 3,
            out_specs=vmem,
            scratch_shapes=[
                pltpu.VMEM((chunks, GROUP * band, coeffs), F32),
                pltpu.VMEM((rows, cells), F32),
                pltpu.VMEM((rows, cells), F32),
                pltpu.VMEM((chunks, n, band, wide), F32),
                pltpu.VMEM((chunks, n, band, wide), F32),
                pltpu.VMEM((chunks, cells, wide), F32),
                pltpu.VMEM((chunks, n, band, wide), F32),
                pltpu.VMEM((chunks, n, band, wide), F32),
                pltpu.VMEM((chunks, wide // LANES, LANES), F32),
                pltpu.VMEM((chunks, n, wide // LANES, LANES), F32),
                pltpu.VMEM((coeffs, cells // 2), BF16),
                pltpu.VMEM((coeffs, cells // 2), BF16),
                pltpu.VMEM((cells // 2, coeffs), BF16),
                pltpu.VMEM((cells // 2, coeffs), BF16),
                pltpu.VMEM((cells, LANES), F32),
                pltpu.VMEM((cells, LANES), F32),
                pltpu.VMEM((2 * GROUP * band, cells // 2), BF16),
                pltpu.VMEM((2 * GROUP * band, cells // 2), BF16),
                pltpu.VMEM((coeffs, 2 * wide), BF16),
                pltpu.VMEM((coeffs, 2 * wide), BF16),
                pltpu.VMEM((cells // 2, 2 * wide), BF16),
                pltpu.VMEM((cells // 2, 2 * wide), BF16),
            ]
            + [dma((chunks,)), dma((2,))] + [dma((chunks,))] * 6,
            compiler_params=pltpu.CompilerParams(
                collective_id=0, has_side_effects=True, vmem_limit_bytes=44 * 1024 * 1024
            ),
        )(
            *(
                pltpu.with_memory_space_constraint(value, pltpu.HBM)
                for value in (spectral.reshape(chunks, GROUP * band, coeffs), coupling, quadratic)
            )
        )
        return result.reshape(levels, band, coeffs)

    spec = P("member", "band", None)
    field = P(("member", "band"), None)
    return jax.shard_map(
        on_device,
        mesh=mesh,
        in_specs=(spec, field, field),
        out_specs=spec,
        check_vma=False,
    )
```

```python
import functools
import math

import jax
import jax.numpy as jnp
from jax import lax
from jax.experimental import pallas as pl
from jax.experimental.pallas import tpu as pltpu
from jax.sharding import PartitionSpec as P

MESH = pl.DeviceIdType.MESH
F32 = jnp.float32
BF16 = jnp.bfloat16
GROUP = 2
AHEAD = 3
ANALYZE = 3
FINISH = 6
LANES = 128
ORDER = ((1, 2), (0, 3), (1, 1), (0, 2), (1, 0), (0, 1), (1, 3), (0, 0))


SINE = (-1.6666666666666666e-01, 8.3333333333333333e-03, -1.9841269841269841e-04, 2.7557319223985891e-06)
COSINE = (-0.5, 4.1666666666666667e-02, -1.3888888888888889e-03, 2.4801587301587302e-05, -2.7557319223985891e-07)


def turn(index, cells):
    quarter = cells // 4
    index = lax.rem(index, cells)
    which = index // quarter
    angle = (index - which * quarter - quarter // 2).astype(F32) * (2.0 * math.pi / cells)
    square = angle * angle

    def series(terms):
        total = terms[-1]
        for term in terms[-2::-1]:
            total = total * square + term
        return total * square + 1.0

    cosine = series(COSINE) * math.sqrt(0.5)
    sine = series(SINE) * angle * math.sqrt(0.5)
    plus, minus = cosine + sine, cosine - sine
    cos_sign = jnp.where((which == 1) | (which == 2), -1.0, 1.0)
    sin_sign = jnp.where(which >= 2, -1.0, 1.0)
    odd = (which == 1) | (which == 3)
    return jnp.where(odd, plus, minus) * cos_sign, jnp.where(odd, minus, plus) * sin_sign


def split(value):
    high = value.astype(BF16)
    return high, (value - high.astype(F32)).astype(BF16)


def dot3(a_high, a_low, b_high, b_low):
    dot = functools.partial(jnp.dot, preferred_element_type=F32)
    return dot(a_high, b_high) + dot(a_low, b_high) + dot(a_high, b_low)


def settle(both, me, band, points, start, coeffs):
    rows, width = both.shape[0] // 2, both.shape[1]
    half = coeffs // 2

    def weight(index):
        return jnp.where((index == 0) | (index == half), 1.0, 2.0)

    y_index = lax.broadcasted_iota(jnp.int32, (rows, width), 1) + start
    x_index = lax.rem(lax.broadcasted_iota(jnp.int32, (rows, width), 0), band) + me * band
    done = jnp.where(lax.rem(y_index, 2) == 0, both[:rows], both[rows:])
    return done * (weight(x_index) * weight(y_index) * (half / points))


def last_kernel(band, points, ready, left_high, left_low, tall_high, tall_low, out, last, sem):
    before, coeffs = ready.shape[0], ready.shape[2]
    me = lax.axis_index("band")
    copies = [pltpu.make_async_copy(ready, out.at[pl.ds(0, before)], sem.at[0])]
    copies[0].start()
    tile = 2 * LANES
    for t in range(coeffs // tile):
        lanes = pl.ds(t * tile, tile)
        both = dot3(left_high[...], left_low[...], tall_high[:, lanes], tall_low[:, lanes])
        last[t] = settle(both, me, band, points, t * tile, coeffs)
        copies.append(pltpu.make_async_copy(last.at[t], out.at[before, :, lanes], sem.at[t + 1]))
        copies[-1].start()
    for copy in copies:
        copy.wait()


def kernel(
    n,
    spectral,
    coupling_hbm,
    quadratic_hbm,
    out,
    left_high,
    left_low,
    tall_high,
    tall_low,
    x_in,
    coupling,
    quadratic,
    send1,
    recv1,
    product,
    send2,
    recv2,
    part_out,
    part_in,
    wide_high,
    wide_low,
    gain,
    bend,
    right_high,
    right_low,
    down_high,
    down_low,
    in_sem,
    field_sem,
    send1_sem,
    recv1_sem,
    send2_sem,
    recv2_sem,
    part_send_sem,
    part_recv_sem,
):
    chunks, band, coeffs = x_in.shape[0], send1.shape[2], x_in.shape[2]
    half = coeffs // 2
    rows, cells = coupling.shape
    points = float(cells * cells)
    fold = cells // 2
    wide = GROUP * rows
    me = lax.axis_index("band")
    chip, core = me // 2, lax.rem(me, 2)
    ring = n // 4

    def at(dy, dx, dc):
        y, x = lax.rem(chip // ring + dy, 2), lax.rem(chip + dx, ring)
        return 2 * (ring * y + x) + lax.rem(core + dc, 2)

    others = [at(dy, dx, dc) for dy, dx in ORDER for dc in range(2) if (dy, dx, dc) != (0, 0, 0)]

    for c in range(chunks):
        pltpu.make_async_copy(spectral.at[c], x_in.at[c], in_sem.at[c]).start()
    pltpu.make_async_copy(coupling_hbm, coupling, field_sem.at[0]).start()
    pltpu.make_async_copy(quadratic_hbm, quadratic, field_sem.at[1]).start()

    barrier = pltpu.get_barrier_semaphore()

    @pl.loop(1, n)
    def _(k):
        pl.semaphore_signal(
            barrier, inc=1, device_id={"band": lax.rem(me + k, n)}, device_id_type=MESH
        )

    def count(shape, axis):
        return lax.broadcasted_iota(jnp.int32, shape, axis)

    fine = (half, LANES)
    cos_q, sin_q = turn(count(fine, 0) * count(fine, 1), cells)
    cos_q = cos_q.reshape(half // 8, 8, LANES)
    sin_q = sin_q.reshape(half // 8, 8, LANES)
    for step in range(fold // LANES):
        lanes = pl.ds(step * LANES, LANES)
        cos_s, sin_s = turn(count((8, LANES), 0) * (step * LANES), cells)
        cos_s, sin_s = cos_s[None], sin_s[None]
        cosine = (cos_q * cos_s - sin_q * sin_s).reshape(half, LANES)
        sine = (sin_q * cos_s + cos_q * sin_s).reshape(half, LANES)
        wide_high[pl.ds(0, half), lanes], wide_low[pl.ds(0, half), lanes] = split(cosine)
        wide_high[pl.ds(half, half), lanes], wide_low[pl.ds(half, half), lanes] = split(sine)

    low_half = lax.broadcasted_iota(jnp.int32, (band, LANES), 1) < rows

    def send_one(source, target, c, send_sem, recv_sem, other):
        pltpu.make_async_remote_copy(
            src_ref=source.at[c, other],
            dst_ref=target.at[c, me],
            send_sem=send_sem.at[c],
            recv_sem=recv_sem.at[c],
            device_id={"band": other},
            device_id_type=MESH,
        ).start()

    def send(source, target, c, send_sem, recv_sem):
        for other in others:
            send_one(source, target, c, send_sem, recv_sem, other)
        target[c, me] = source[c, me]

    def arrivals(source, target, c, send_sem, recv_sem):
        rest = pl.ds(0, n - 1)
        return pltpu.make_async_remote_copy(
            src_ref=source.at[c, rest],
            dst_ref=target.at[c, rest],
            send_sem=send_sem.at[c],
            recv_sem=recv_sem.at[c],
            device_id={"band": lax.rem(me + 1, n)},
            device_id_type=MESH,
        )

    def sums_of(c):
        rest = pl.ds(0, n - 1)
        return pltpu.make_async_remote_copy(
            src_ref=part_in.at[c, rest],
            dst_ref=part_in.at[c, rest],
            send_sem=part_send_sem.at[c],
            recv_sem=part_recv_sem.at[c],
            device_id={"band": lax.rem(me + 1, n)},
            device_id_type=MESH,
        )

    first = (send1, recv1)
    second = (send2, recv2)

    @pl.loop(0, chunks)
    def _(c):
        pltpu.make_async_copy(spectral.at[c], x_in.at[c], in_sem.at[c]).wait()
        value = x_in[c]
        even_k = lax.rem(count(value.shape, 1), 2) == 0
        parts = jnp.concatenate([jnp.where(even_k, value, 0.0), jnp.where(even_k, 0.0, value)])
        x_high, x_low = split(parts)
        tile = 2 * LANES
        for j in range(fold // tile):
            lanes = pl.ds(j * tile, tile)
            both = dot3(x_high, x_low, wide_high[:, lanes], wide_low[:, lanes])
            even_sum, odd_sum = both[: GROUP * band], both[GROUP * band :]
            for side, section in enumerate((even_sum + odd_sum, even_sum - odd_sum)):
                for level in range(0, GROUP, 2):
                    for t in range(tile // LANES):
                        part = slice(t * LANES, (t + 1) * LANES)
                        even = section[level * band : (level + 1) * band, part]
                        odd = section[(level + 1) * band : (level + 2) * band, part]
                        target = (side * fold + j * tile + t * LANES) // rows
                        place = pl.ds(level * rows, LANES)
                        send1[c, target, :, place] = jnp.where(
                            low_half, even, pltpu.roll(odd, rows, 1)
                        )
                        send1[c, target + 1, :, place] = jnp.where(
                            low_half, pltpu.roll(even, rows, 1), odd
                        )

        @pl.when(c == 0)
        def _():
            pl.semaphore_wait(barrier, n - 1)

        @pl.when(c < AHEAD)
        def _():
            send(*first, c, send1_sem, recv1_sem)

    fine = (LANES, half)
    cos_q, sin_q = turn(count(fine, 0) * count(fine, 1), cells)
    for step in range(fold // LANES):
        points_here = pl.ds(step * LANES, LANES)
        cos_s, sin_s = turn(count((8, half), 1) * (step * LANES), cells)
        cos_s, sin_s = cos_s[:1], sin_s[:1]
        cosine = cos_q * cos_s - sin_q * sin_s
        sine = sin_q * cos_s + cos_q * sin_s
        (tall_high[points_here, pl.ds(0, half)], tall_low[points_here, pl.ds(0, half)]) = split(
            cosine
        )
        (
            tall_high[points_here, pl.ds(half, half)],
            tall_low[points_here, pl.ds(half, half)],
        ) = split(sine)

    pltpu.make_async_copy(coupling_hbm, coupling, field_sem.at[0]).wait()
    pltpu.make_async_copy(quadratic_hbm, quadratic, field_sem.at[1]).wait()

    for step in range(cells // LANES):
        here = pl.ds(step * LANES, LANES)
        field = coupling[:, here] * (1.0 / half)
        gain[here, :] = jnp.concatenate([field, field], axis=0).T
        field = quadratic[:, here]
        bend[here, :] = jnp.concatenate([field, field], axis=0).T

    def synthesize(c):
        arrivals(*first, c, send1_sem, recv1_sem).wait_recv()
        value = recv1[c].reshape(coeffs, wide)
        even_k = lax.rem(count(value.shape, 0), 2) == 0
        for side, part in enumerate((jnp.where(even_k, value, 0.0), jnp.where(even_k, 0.0, value))):
            lanes = pl.ds(side * wide, wide)
            right_high[:, lanes], right_low[:, lanes] = split(part)
        both = dot3(tall_high[...], tall_low[...], right_high[...], right_low[...])
        even_sum, odd_sum = both[:, :wide], both[:, wide:]
        sums = 0.0
        for side, grid in enumerate((even_sum + odd_sum, even_sum - odd_sum)):
            here = pl.ds(side * fold, fold)
            value = jnp.concatenate([gain[here]] * (wide // LANES), axis=1) * grid
            product[c, here] = value
            sums = sums + jnp.sum(value * value, axis=0, keepdims=True)
        for t in range(wide // LANES):
            part_out[c, pl.ds(t, 1), :] = sums[:, t * LANES : (t + 1) * LANES]

        for other in others:
            pltpu.make_async_remote_copy(
                src_ref=part_out.at[c],
                dst_ref=part_in.at[c, me],
                send_sem=part_send_sem.at[c],
                recv_sem=part_recv_sem.at[c],
                device_id={"band": other},
                device_id_type=MESH,
            ).start()
        part_in[c, me] = part_out[c]

    def analyze(c):
        sums_of(c).wait_recv()
        sums = part_in[c, 0]
        for source in range(1, n):
            sums = sums + part_in[c, source]
        left = lax.broadcasted_iota(jnp.int32, sums.shape, 1) < rows
        total = jnp.where(
            left,
            jnp.sum(jnp.where(left, sums, 0.0), axis=1, keepdims=True),
            jnp.sum(jnp.where(left, 0.0, sums), axis=1, keepdims=True),
        )
        scale = 1.0 / jnp.sqrt(total * (1.0 / points) + 1e-06)
        scale = jnp.concatenate([scale[t : t + 1] for t in range(wide // LANES)], axis=1)
        halves = []
        for side in range(2):
            here = pl.ds(side * fold, fold)
            scaled = product[c, here] * scale
            weight = jnp.concatenate([bend[here]] * (wide // LANES), axis=1)
            halves.append(scaled + weight * scaled * scaled)
        for side, part in enumerate((halves[0] + halves[1], halves[0] - halves[1])):
            lanes = pl.ds(side * wide, wide)
            down_high[:, lanes], down_low[:, lanes] = split(part)
        both = dot3(wide_high[...], wide_low[...], down_high[...], down_low[...])
        even_k = lax.rem(count((coeffs, wide), 0), 2) == 0
        back = jnp.where(even_k, both[:, :wide], both[:, wide:])
        send2[c] = back.reshape(n, band, wide)
        send(*second, c, send2_sem, recv2_sem)

    def finish(c):
        arrivals(*first, c, send1_sem, recv1_sem).wait_send()
        arrivals(*second, c, send2_sem, recv2_sem).wait_send()
        sums_of(c).wait_send()
        arrivals(*second, c, send2_sem, recv2_sem).wait_recv()
        for level in range(0, GROUP, 2):
            place = pl.ds(level * rows, LANES)
            for t in range(fold // LANES):
                lanes = pl.ds(t * LANES, LANES)
                turned = []
                for near in (2 * t, 2 * t + fold // rows):
                    even = recv2[c, near, :, place]
                    odd = recv2[c, near + 1, :, place]
                    turned.append(
                        (
                            jnp.where(low_half, even, pltpu.roll(odd, rows, 1)),
                            jnp.where(low_half, pltpu.roll(even, rows, 1), odd),
                        )
                    )
                for which in range(2):
                    near, far = turned[0][which], turned[1][which]
                    here = (level + which) * band
                    for side, value in enumerate((near + far, near - far)):
                        there = pl.ds(side * GROUP * band + here, band)
                        left_high[there, lanes], left_low[there, lanes] = split(value)

        @pl.when(c < chunks - 1)
        def _():
            both = dot3(left_high[...], left_low[...], tall_high[...], tall_low[...])
            out[c] = settle(both, me, band, points, 0, coeffs)

    @pl.loop(0, chunks + FINISH)
    def _(t):
        @pl.when(t < chunks)
        def _():
            synthesize(t)

        @pl.when(t + AHEAD < chunks)
        def _():
            send(*first, t + AHEAD, send1_sem, recv1_sem)

        @pl.when((t >= ANALYZE) & (t < chunks + ANALYZE))
        def _():
            analyze(t - ANALYZE)

        @pl.when(t >= FINISH)
        def _():
            finish(t - FINISH)


def solution(mesh):
    n = mesh.shape["band"]

    def on_device(spectral, coupling, quadratic):
        levels, band, coeffs = spectral.shape
        rows, cells = coupling.shape
        chunks = levels // GROUP
        wide = GROUP * rows
        dma = pltpu.SemaphoreType.DMA
        vmem = pl.BlockSpec(memory_space=pltpu.VMEM)
        hbm = pl.BlockSpec(memory_space=pltpu.HBM)
        parts = pl.pallas_call(
            functools.partial(kernel, n),
            out_shape=(
                pltpu.VMEM((chunks - 1, GROUP * band, coeffs), F32),
                pltpu.VMEM((2 * GROUP * band, cells // 2), BF16),
                pltpu.VMEM((2 * GROUP * band, cells // 2), BF16),
                pltpu.VMEM((cells // 2, coeffs), BF16),
                pltpu.VMEM((cells // 2, coeffs), BF16),
            ),
            in_specs=[hbm] * 3,
            out_specs=(vmem,) * 5,
            scratch_shapes=[
                pltpu.VMEM((chunks, GROUP * band, coeffs), F32),
                pltpu.VMEM((rows, cells), F32),
                pltpu.VMEM((rows, cells), F32),
                pltpu.VMEM((chunks, n, band, wide), F32),
                pltpu.VMEM((chunks, n, band, wide), F32),
                pltpu.VMEM((chunks, cells, wide), F32),
                pltpu.VMEM((chunks, n, band, wide), F32),
                pltpu.VMEM((chunks, n, band, wide), F32),
                pltpu.VMEM((chunks, wide // LANES, LANES), F32),
                pltpu.VMEM((chunks, n, wide // LANES, LANES), F32),
                pltpu.VMEM((coeffs, cells // 2), BF16),
                pltpu.VMEM((coeffs, cells // 2), BF16),
                pltpu.VMEM((cells, LANES), F32),
                pltpu.VMEM((cells, LANES), F32),
                pltpu.VMEM((coeffs, 2 * wide), BF16),
                pltpu.VMEM((coeffs, 2 * wide), BF16),
                pltpu.VMEM((cells // 2, 2 * wide), BF16),
                pltpu.VMEM((cells // 2, 2 * wide), BF16),
            ]
            + [dma((chunks,)), dma((2,))] + [dma((chunks,))] * 6,
            compiler_params=pltpu.CompilerParams(
                collective_id=0, has_side_effects=True, vmem_limit_bytes=44 * 1024 * 1024
            ),
        )(
            *(
                pltpu.with_memory_space_constraint(value, pltpu.HBM)
                for value in (spectral.reshape(chunks, GROUP * band, coeffs), coupling, quadratic)
            )
        )
        result = pl.pallas_call(
            functools.partial(last_kernel, band, float(cells * cells)),
            out_shape=jax.ShapeDtypeStruct((chunks, GROUP * band, coeffs), F32),
            in_specs=[vmem] * 5,
            out_specs=pl.BlockSpec(memory_space=pltpu.HBM),
            scratch_shapes=[
                pltpu.VMEM((coeffs // (2 * LANES), GROUP * band, 2 * LANES), F32),
                dma((1 + coeffs // (2 * LANES),)),
            ],
            compiler_params=pltpu.CompilerParams(vmem_limit_bytes=16 * 1024 * 1024),
        )(*(pltpu.with_memory_space_constraint(part, pltpu.VMEM) for part in parts))
        return result.reshape(levels, band, coeffs)

    spec = P("member", "band", None)
    field = P(("member", "band"), None)
    return jax.shard_map(
        on_device,
        mesh=mesh,
        in_specs=(spec, field, field),
        out_specs=spec,
        check_vma=False,
    )
```

```python
import functools
import math

import jax
import jax.numpy as jnp
from jax import lax
from jax.experimental import pallas as pl
from jax.experimental.pallas import tpu as pltpu
from jax.sharding import PartitionSpec as P

MESH = pl.DeviceIdType.MESH
F32 = jnp.float32
BF16 = jnp.bfloat16
GROUP = 2
AHEAD = 3
ANALYZE = 3
FINISH = 6
LANES = 128
ORDER = ((1, 1), (0, 3), (1, 2), (0, 1), (1, 3), (0, 2), (1, 0), (0, 0))


SINE = (-1.6666666666666666e-01, 8.3333333333333333e-03, -1.9841269841269841e-04, 2.7557319223985891e-06)
COSINE = (-0.5, 4.1666666666666667e-02, -1.3888888888888889e-03, 2.4801587301587302e-05, -2.7557319223985891e-07)


def turn(index, cells):
    quarter = cells // 4
    index = lax.rem(index, cells)
    which = index // quarter
    angle = (index - which * quarter - quarter // 2).astype(F32) * (2.0 * math.pi / cells)
    square = angle * angle

    def series(terms):
        total = terms[-1]
        for term in terms[-2::-1]:
            total = total * square + term
        return total * square + 1.0

    cosine = series(COSINE) * math.sqrt(0.5)
    sine = series(SINE) * angle * math.sqrt(0.5)
    plus, minus = cosine + sine, cosine - sine
    cos_sign = jnp.where((which == 1) | (which == 2), -1.0, 1.0)
    sin_sign = jnp.where(which >= 2, -1.0, 1.0)
    odd = (which == 1) | (which == 3)
    return jnp.where(odd, plus, minus) * cos_sign, jnp.where(odd, minus, plus) * sin_sign


def split(value):
    high = value.astype(BF16)
    return high, (value - high.astype(F32)).astype(BF16)


def dot3(a_high, a_low, b_high, b_low):
    dot = functools.partial(jnp.dot, preferred_element_type=F32)
    return dot(a_high, b_high) + dot(a_low, b_high) + dot(a_high, b_low)


def settle(both, me, band, points, start, coeffs):
    rows, width = both.shape[0] // 2, both.shape[1]
    half = coeffs // 2

    def weight(index):
        return jnp.where((index == 0) | (index == half), 1.0, 2.0)

    y_index = lax.broadcasted_iota(jnp.int32, (rows, width), 1) + start
    x_index = lax.rem(lax.broadcasted_iota(jnp.int32, (rows, width), 0), band) + me * band
    done = jnp.where(lax.rem(y_index, 2) == 0, both[:rows], both[rows:])
    return done * (weight(x_index) * weight(y_index) * (half / points))


def last_kernel(band, points, ready, left_high, left_low, tall_high, tall_low, out, last, sem):
    before, coeffs = ready.shape[0], ready.shape[2]
    me = lax.axis_index("band")
    copies = [pltpu.make_async_copy(ready, out.at[pl.ds(0, before)], sem.at[0])]
    copies[0].start()
    tile = 2 * LANES
    for t in range(coeffs // tile):
        lanes = pl.ds(t * tile, tile)
        both = dot3(left_high[...], left_low[...], tall_high[:, lanes], tall_low[:, lanes])
        last[t] = settle(both, me, band, points, t * tile, coeffs)
        copies.append(pltpu.make_async_copy(last.at[t], out.at[before, :, lanes], sem.at[t + 1]))
        copies[-1].start()
    for copy in copies:
        copy.wait()


def kernel(
    n,
    spectral,
    coupling_hbm,
    quadratic_hbm,
    out,
    left_high,
    left_low,
    tall_high,
    tall_low,
    x_in,
    coupling,
    quadratic,
    send1,
    recv1,
    product,
    send2,
    recv2,
    part_out,
    part_in,
    wide_high,
    wide_low,
    gain,
    bend,
    right_high,
    right_low,
    down_high,
    down_low,
    in_sem,
    field_sem,
    send1_sem,
    recv1_sem,
    send2_sem,
    recv2_sem,
    part_send_sem,
    part_recv_sem,
):
    chunks, band, coeffs = x_in.shape[0], send1.shape[2], x_in.shape[2]
    half = coeffs // 2
    rows, cells = coupling.shape
    points = float(cells * cells)
    fold = cells // 2
    wide = GROUP * rows
    me = lax.axis_index("band")
    chip, core = me // 2, lax.rem(me, 2)
    ring = n // 4

    def at(dy, dx, dc):
        y, x = lax.rem(chip // ring + dy, 2), lax.rem(chip + dx, ring)
        return 2 * (ring * y + x) + lax.rem(core + dc, 2)

    others = [at(dy, dx, dc) for dy, dx in ORDER for dc in range(2) if (dy, dx, dc) != (0, 0, 0)]

    for c in range(chunks):
        pltpu.make_async_copy(spectral.at[c], x_in.at[c], in_sem.at[c]).start()
    pltpu.make_async_copy(coupling_hbm, coupling, field_sem.at[0]).start()
    pltpu.make_async_copy(quadratic_hbm, quadratic, field_sem.at[1]).start()

    barrier = pltpu.get_barrier_semaphore()

    @pl.loop(1, n)
    def _(k):
        pl.semaphore_signal(
            barrier, inc=1, device_id={"band": lax.rem(me + k, n)}, device_id_type=MESH
        )

    def count(shape, axis):
        return lax.broadcasted_iota(jnp.int32, shape, axis)

    fine = (half, LANES)
    cos_q, sin_q = turn(count(fine, 0) * count(fine, 1), cells)
    cos_q = cos_q.reshape(half // 8, 8, LANES)
    sin_q = sin_q.reshape(half // 8, 8, LANES)
    for step in range(fold // LANES):
        lanes = pl.ds(step * LANES, LANES)
        cos_s, sin_s = turn(count((8, LANES), 0) * (step * LANES), cells)
        cos_s, sin_s = cos_s[None], sin_s[None]
        cosine = (cos_q * cos_s - sin_q * sin_s).reshape(half, LANES)
        sine = (sin_q * cos_s + cos_q * sin_s).reshape(half, LANES)
        wide_high[pl.ds(0, half), lanes], wide_low[pl.ds(0, half), lanes] = split(cosine)
        wide_high[pl.ds(half, half), lanes], wide_low[pl.ds(half, half), lanes] = split(sine)

    low_half = lax.broadcasted_iota(jnp.int32, (band, LANES), 1) < rows

    def send_one(source, target, c, send_sem, recv_sem, other):
        pltpu.make_async_remote_copy(
            src_ref=source.at[c, other],
            dst_ref=target.at[c, me],
            send_sem=send_sem.at[c],
            recv_sem=recv_sem.at[c],
            device_id={"band": other},
            device_id_type=MESH,
        ).start()

    def send(source, target, c, send_sem, recv_sem):
        for other in others:
            send_one(source, target, c, send_sem, recv_sem, other)
        target[c, me] = source[c, me]

    def arrivals(source, target, c, send_sem, recv_sem):
        rest = pl.ds(0, n - 1)
        return pltpu.make_async_remote_copy(
            src_ref=source.at[c, rest],
            dst_ref=target.at[c, rest],
            send_sem=send_sem.at[c],
            recv_sem=recv_sem.at[c],
            device_id={"band": lax.rem(me + 1, n)},
            device_id_type=MESH,
        )

    def sums_of(c):
        rest = pl.ds(0, n - 1)
        return pltpu.make_async_remote_copy(
            src_ref=part_in.at[c, rest],
            dst_ref=part_in.at[c, rest],
            send_sem=part_send_sem.at[c],
            recv_sem=part_recv_sem.at[c],
            device_id={"band": lax.rem(me + 1, n)},
            device_id_type=MESH,
        )

    first = (send1, recv1)
    second = (send2, recv2)

    @pl.loop(0, chunks)
    def _(c):
        pltpu.make_async_copy(spectral.at[c], x_in.at[c], in_sem.at[c]).wait()
        value = x_in[c]
        even_k = lax.rem(count(value.shape, 1), 2) == 0
        parts = jnp.concatenate([jnp.where(even_k, value, 0.0), jnp.where(even_k, 0.0, value)])
        x_high, x_low = split(parts)
        tile = 2 * LANES
        for j in range(fold // tile):
            lanes = pl.ds(j * tile, tile)
            both = dot3(x_high, x_low, wide_high[:, lanes], wide_low[:, lanes])
            even_sum, odd_sum = both[: GROUP * band], both[GROUP * band :]
            for side, section in enumerate((even_sum + odd_sum, even_sum - odd_sum)):
                for level in range(0, GROUP, 2):
                    for t in range(tile // LANES):
                        part = slice(t * LANES, (t + 1) * LANES)
                        even = section[level * band : (level + 1) * band, part]
                        odd = section[(level + 1) * band : (level + 2) * band, part]
                        target = (side * fold + j * tile + t * LANES) // rows
                        place = pl.ds(level * rows, LANES)
                        send1[c, target, :, place] = jnp.where(
                            low_half, even, pltpu.roll(odd, rows, 1)
                        )
                        send1[c, target + 1, :, place] = jnp.where(
                            low_half, pltpu.roll(even, rows, 1), odd
                        )

        @pl.when(c == 0)
        def _():
            pl.semaphore_wait(barrier, n - 1)

        @pl.when(c < AHEAD)
        def _():
            send(*first, c, send1_sem, recv1_sem)

    fine = (LANES, half)
    cos_q, sin_q = turn(count(fine, 0) * count(fine, 1), cells)
    for step in range(fold // LANES):
        points_here = pl.ds(step * LANES, LANES)
        cos_s, sin_s = turn(count((8, half), 1) * (step * LANES), cells)
        cos_s, sin_s = cos_s[:1], sin_s[:1]
        cosine = cos_q * cos_s - sin_q * sin_s
        sine = sin_q * cos_s + cos_q * sin_s
        (tall_high[points_here, pl.ds(0, half)], tall_low[points_here, pl.ds(0, half)]) = split(
            cosine
        )
        (
            tall_high[points_here, pl.ds(half, half)],
            tall_low[points_here, pl.ds(half, half)],
        ) = split(sine)

    pltpu.make_async_copy(coupling_hbm, coupling, field_sem.at[0]).wait()
    pltpu.make_async_copy(quadratic_hbm, quadratic, field_sem.at[1]).wait()

    for step in range(cells // LANES):
        here = pl.ds(step * LANES, LANES)
        field = coupling[:, here] * (1.0 / half)
        gain[here, :] = jnp.concatenate([field, field], axis=0).T
        field = quadratic[:, here]
        bend[here, :] = jnp.concatenate([field, field], axis=0).T

    def synthesize(c):
        arrivals(*first, c, send1_sem, recv1_sem).wait_recv()
        value = recv1[c].reshape(coeffs, wide)
        even_k = lax.rem(count(value.shape, 0), 2) == 0
        for side, part in enumerate((jnp.where(even_k, value, 0.0), jnp.where(even_k, 0.0, value))):
            lanes = pl.ds(side * wide, wide)
            right_high[:, lanes], right_low[:, lanes] = split(part)
        both = dot3(tall_high[...], tall_low[...], right_high[...], right_low[...])
        even_sum, odd_sum = both[:, :wide], both[:, wide:]
        sums = 0.0
        for side, grid in enumerate((even_sum + odd_sum, even_sum - odd_sum)):
            here = pl.ds(side * fold, fold)
            value = jnp.concatenate([gain[here]] * (wide // LANES), axis=1) * grid
            product[c, here] = value
            sums = sums + jnp.sum(value * value, axis=0, keepdims=True)
        for t in range(wide // LANES):
            part_out[c, pl.ds(t, 1), :] = sums[:, t * LANES : (t + 1) * LANES]

        for other in others:
            pltpu.make_async_remote_copy(
                src_ref=part_out.at[c],
                dst_ref=part_in.at[c, me],
                send_sem=part_send_sem.at[c],
                recv_sem=part_recv_sem.at[c],
                device_id={"band": other},
                device_id_type=MESH,
            ).start()
        part_in[c, me] = part_out[c]

    def analyze(c):
        sums_of(c).wait_recv()
        sums = part_in[c, 0]
        for source in range(1, n):
            sums = sums + part_in[c, source]
        left = lax.broadcasted_iota(jnp.int32, sums.shape, 1) < rows
        total = jnp.where(
            left,
            jnp.sum(jnp.where(left, sums, 0.0), axis=1, keepdims=True),
            jnp.sum(jnp.where(left, 0.0, sums), axis=1, keepdims=True),
        )
        scale = 1.0 / jnp.sqrt(total * (1.0 / points) + 1e-06)
        scale = jnp.concatenate([scale[t : t + 1] for t in range(wide // LANES)], axis=1)
        halves = []
        for side in range(2):
            here = pl.ds(side * fold, fold)
            scaled = product[c, here] * scale
            weight = jnp.concatenate([bend[here]] * (wide // LANES), axis=1)
            halves.append(scaled + weight * scaled * scaled)
        for side, part in enumerate((halves[0] + halves[1], halves[0] - halves[1])):
            lanes = pl.ds(side * wide, wide)
            down_high[:, lanes], down_low[:, lanes] = split(part)
        both = dot3(wide_high[...], wide_low[...], down_high[...], down_low[...])
        even_k = lax.rem(count((coeffs, wide), 0), 2) == 0
        back = jnp.where(even_k, both[:, :wide], both[:, wide:])
        send2[c] = back.reshape(n, band, wide)
        send(*second, c, send2_sem, recv2_sem)

    def finish(c):
        arrivals(*first, c, send1_sem, recv1_sem).wait_send()
        arrivals(*second, c, send2_sem, recv2_sem).wait_send()
        sums_of(c).wait_send()
        arrivals(*second, c, send2_sem, recv2_sem).wait_recv()
        for level in range(0, GROUP, 2):
            place = pl.ds(level * rows, LANES)
            for t in range(fold // LANES):
                lanes = pl.ds(t * LANES, LANES)
                turned = []
                for near in (2 * t, 2 * t + fold // rows):
                    even = recv2[c, near, :, place]
                    odd = recv2[c, near + 1, :, place]
                    turned.append(
                        (
                            jnp.where(low_half, even, pltpu.roll(odd, rows, 1)),
                            jnp.where(low_half, pltpu.roll(even, rows, 1), odd),
                        )
                    )
                for which in range(2):
                    near, far = turned[0][which], turned[1][which]
                    here = (level + which) * band
                    for side, value in enumerate((near + far, near - far)):
                        there = pl.ds(side * GROUP * band + here, band)
                        left_high[there, lanes], left_low[there, lanes] = split(value)

        @pl.when(c < chunks - 1)
        def _():
            both = dot3(left_high[...], left_low[...], tall_high[...], tall_low[...])
            out[c] = settle(both, me, band, points, 0, coeffs)

    @pl.loop(0, chunks + FINISH)
    def _(t):
        @pl.when(t < chunks)
        def _():
            synthesize(t)

        @pl.when(t + AHEAD < chunks)
        def _():
            send(*first, t + AHEAD, send1_sem, recv1_sem)

        @pl.when((t >= ANALYZE) & (t < chunks + ANALYZE))
        def _():
            analyze(t - ANALYZE)

        @pl.when(t >= FINISH)
        def _():
            finish(t - FINISH)


def solution(mesh):
    n = mesh.shape["band"]

    def on_device(spectral, coupling, quadratic):
        levels, band, coeffs = spectral.shape
        rows, cells = coupling.shape
        chunks = levels // GROUP
        wide = GROUP * rows
        dma = pltpu.SemaphoreType.DMA
        vmem = pl.BlockSpec(memory_space=pltpu.VMEM)
        hbm = pl.BlockSpec(memory_space=pltpu.HBM)
        parts = pl.pallas_call(
            functools.partial(kernel, n),
            out_shape=(
                pltpu.VMEM((chunks - 1, GROUP * band, coeffs), F32),
                pltpu.VMEM((2 * GROUP * band, cells // 2), BF16),
                pltpu.VMEM((2 * GROUP * band, cells // 2), BF16),
                pltpu.VMEM((cells // 2, coeffs), BF16),
                pltpu.VMEM((cells // 2, coeffs), BF16),
            ),
            in_specs=[hbm] * 3,
            out_specs=(vmem,) * 5,
            scratch_shapes=[
                pltpu.VMEM((chunks, GROUP * band, coeffs), F32),
                pltpu.VMEM((rows, cells), F32),
                pltpu.VMEM((rows, cells), F32),
                pltpu.VMEM((chunks, n, band, wide), F32),
                pltpu.VMEM((chunks, n, band, wide), F32),
                pltpu.VMEM((chunks, cells, wide), F32),
                pltpu.VMEM((chunks, n, band, wide), F32),
                pltpu.VMEM((chunks, n, band, wide), F32),
                pltpu.VMEM((chunks, wide // LANES, LANES), F32),
                pltpu.VMEM((chunks, n, wide // LANES, LANES), F32),
                pltpu.VMEM((coeffs, cells // 2), BF16),
                pltpu.VMEM((coeffs, cells // 2), BF16),
                pltpu.VMEM((cells, LANES), F32),
                pltpu.VMEM((cells, LANES), F32),
                pltpu.VMEM((coeffs, 2 * wide), BF16),
                pltpu.VMEM((coeffs, 2 * wide), BF16),
                pltpu.VMEM((cells // 2, 2 * wide), BF16),
                pltpu.VMEM((cells // 2, 2 * wide), BF16),
            ]
            + [dma((chunks,)), dma((2,))] + [dma((chunks,))] * 6,
            compiler_params=pltpu.CompilerParams(
                collective_id=0, has_side_effects=True, vmem_limit_bytes=44 * 1024 * 1024
            ),
        )(
            *(
                pltpu.with_memory_space_constraint(value, pltpu.HBM)
                for value in (spectral.reshape(chunks, GROUP * band, coeffs), coupling, quadratic)
            )
        )
        result = pl.pallas_call(
            functools.partial(last_kernel, band, float(cells * cells)),
            out_shape=jax.ShapeDtypeStruct((chunks, GROUP * band, coeffs), F32),
            in_specs=[vmem] * 5,
            out_specs=pl.BlockSpec(memory_space=pltpu.HBM),
            scratch_shapes=[
                pltpu.VMEM((coeffs // (2 * LANES), GROUP * band, 2 * LANES), F32),
                dma((1 + coeffs // (2 * LANES),)),
            ],
            compiler_params=pltpu.CompilerParams(vmem_limit_bytes=16 * 1024 * 1024),
        )(*(pltpu.with_memory_space_constraint(part, pltpu.VMEM) for part in parts))
        return result.reshape(levels, band, coeffs)

    spec = P("member", "band", None)
    field = P(("member", "band"), None)
    return jax.shard_map(
        on_device,
        mesh=mesh,
        in_specs=(spec, field, field),
        out_specs=spec,
        check_vma=False,
    )
```
